256 devices in a mesh: gx: 8 (over z_lo, core), gy: 32 (over z_hi, y, x).
Axes of the slice: x: 4, y: 4, z: 8 (z_hi: 2, z_lo: 4; z = z_hi * 4 + z_lo), core: 2. Of those that a mesh axis runs over, the one named last changes fastest.
Arguments:
- density: float32 [128, 512, 256], P('gx', 'gy'), may hold values from 0.5 to 2
- momentum: float32 [3, 128, 512, 256], P(None, 'gx', 'gy'), may hold values from -3 to 3
- energy: float32 [128, 512, 256], P('gx', 'gy'), may hold values from 1 to 3
- parcel_mass: float32 [2097152], P(('gx', 'gy')), may hold values from 0.2 to 2
- droplet_velocity: float32 [3, 2097152], P(None, ('gx', 'gy')), may hold values from -4 to 4
- parcel_temp: float32 [2097152], P(('gx', 'gy')), may hold values from 0.1 to 4
- parcel_cell: int32 [3, 2097152], P(None, ('gx', 'gy')), may hold values from 0 to 511, as said below
- parcel_count: int32 [256], P(('gx', 'gy')), may hold values from 2048 to 8192, as said below
Outputs:
- updated_fluid_density: float32 [128, 512, 256], P('gx', 'gy')
- updated_fluid_impulse: float32 [3, 128, 512, 256], P(None, 'gx', 'gy')
- energy_out: float32 [128, 512, 256], P('gx', 'gy')
- moved_state: float32 [5, 2621440], P(None, ('gx', 'gy'))
- moved_cell: int32 [3, 2621440], P(None, ('gx', 'gy'))
- time_step: float32 [], replicated
The draws below stay inside these ranges and needn't reach their ends.
Inputs may be any that keep to these rules, and one draw needn't show every extreme that they name: `parcel_cell`: each row of device d lies in d's block of 16 x 16 x 256 cells or in the layer of cells just beyond one of its four side faces inside the grid, never beyond an edge. Among the live rows of one device at most 512 lie beyond any one face; on every device some face along each of the two axes has exactly 512. `parcel_count`: some devices are full.
All inputs are finite; a program needn't handle non-finite values.
Results may differ from the reference program's by a relative error of at most 0.0003.
Values sent between devices are 32-bit elements; how exact they have to be, the bound alone decides.
A program may use at most 192 MiB of HBM per device.

```python
import math
import jax
import jax.numpy as jnp
from jax import lax

CX = 16
CY = 16
NZ = 256
P_DEV = 8192
MOVE = 512
SLOTS = 10240
NX = 128
NY = 512
PARCELS = 2097152
N_GX = 8
N_GY = 32
DEVICES = 256


def parcel_state_tables(key):
    base = jax.random.fold_in(key, 11)
    keys = jax.random.split(base, 8)
    device = jnp.arange(DEVICES, dtype=jnp.int32)
    col_x = device // N_GY
    col_y = device % N_GY
    partial_parcel_count = jax.random.randint(keys[0], (DEVICES,), P_DEV // 4, P_DEV // 2 + 1, dtype=jnp.int32)
    count = jnp.where(col_x == 0, P_DEV, partial_parcel_count).astype(jnp.int32)
    exists = jnp.stack([col_x > 0, col_x < N_GX - 1, col_y > 0, col_y < N_GY - 1], axis=1)
    loads = jax.random.randint(keys[1], (DEVICES, 4), MOVE // 4, MOVE + 1, dtype=jnp.int32)
    drag_horizontal = jnp.where(col_x < N_GX - 1, 1, 0)
    force_y = jnp.where(col_y < N_GY - 1, 3, 2)
    which = jnp.arange(4, dtype=jnp.int32)[None]
    loads = jnp.where((which == drag_horizontal[:, None]) | (which == force_y[:, None]), MOVE, loads)
    loads = jnp.where(exists, loads, 0)
    ends = jnp.cumsum(loads, axis=1)
    row_index = jnp.arange(P_DEV, dtype=jnp.int32)[None]
    spread = 2 ** 30 // (2 * P_DEV)
    scores = jax.random.randint(keys[2], (DEVICES, P_DEV), 0, spread, dtype=jnp.int32) * P_DEV + row_index
    scores = jnp.where(row_index < count[:, None], scores, 2 ** 30 + row_index)
    order = jnp.argsort(scores, axis=1, stable=True)
    position = jnp.argsort(order, axis=1, stable=True).astype(jnp.int32)
    heading = jnp.sum((position[:, :, None] >= ends[:, None, :]).astype(jnp.int32), axis=2)
    inside_x = jax.random.randint(keys[3], (DEVICES, P_DEV), 0, CX, dtype=jnp.int32) + col_x[:, None] * CX
    inside_y = jax.random.randint(keys[4], (DEVICES, P_DEV), 0, CY, dtype=jnp.int32) + col_y[:, None] * CY
    depth = jax.random.randint(keys[5], (DEVICES, P_DEV), 0, NZ, dtype=jnp.int32)
    cell_x = jnp.where(heading == 0, col_x[:, None] * CX - 1, jnp.where(heading == 1, col_x[:, None] * CX + CX, inside_x))
    cell_y = jnp.where(heading == 2, col_y[:, None] * CY - 1, jnp.where(heading == 3, col_y[:, None] * CY + CY, inside_y))
    cells = jnp.stack([cell_x, cell_y, depth]).reshape(3, DEVICES * P_DEV).astype(jnp.int32)
    return (cells, count)


def draw_parcel_cell(key, part):
    return parcel_state_tables(key)[0]


def draw_parcel_count(key, part):
    return parcel_state_tables(key)[1]


def level_of(stream_key, dims, cuts, smallest, top_value):
    loudness = 1.0
    for dim, blocks in cuts:
        heights = jax.random.uniform(jax.random.fold_in(jax.random.fold_in(stream_key, 6), dim), (blocks,), jnp.float32, smallest / len(cuts), top_value / len(cuts))
        loudness = loudness * jnp.repeat(jnp.exp(heights), dims[dim] // blocks).reshape((-1,) + (1,) * (len(dims) - 1 - dim))
    return loudness


def noise(stream_key, extent, deviation, reach, shards=(), held_as=jnp.bfloat16):
    values = jax.random.normal(stream_key, extent, jnp.float32) * deviation
    if len(shards) > 0:
        values = level_of(stream_key, extent, shards, -0.22, 0.18) * values
    return jnp.clip(values, min=-reach, max=reach).astype(held_as)


def setup_inputs(seed: int = 0) -> dict:
    key_of = jax.random.split(jax.random.key(seed), 9)
    density = jnp.clip(0.5 + 1.5 * jax.random.uniform(key_of[0], (NX, NY, NZ), jnp.float32) ** level_of(key_of[0], (NX, NY, NZ), ((0, 8), (1, 32)), -0.2, 0.2), 0.5, 2.0)
    momentum = noise(key_of[1], (3, NX, NY, NZ), 0.5, 3.0, ((1, 8), (2, 32)), jnp.float32)
    energy = jnp.clip(1.0 + 2.0 * jax.random.uniform(key_of[2], (NX, NY, NZ), jnp.float32) ** level_of(key_of[2], (NX, NY, NZ), ((0, 8), (1, 32)), -0.2, 0.2), 1.0, 3.0)
    parcel_mass = jnp.clip(jnp.exp(math.log(2.0) - 2.3025851 * jax.random.uniform(key_of[3], (PARCELS,), jnp.float32) ** level_of(key_of[3], (PARCELS,), ((0, 256),), -0.2, 0.2)), 0.2, 2.0)
    droplet_velocity = noise(key_of[4], (3, PARCELS), 1.0, 4.0, ((1, 256),), jnp.float32)
    parcel_temp = jnp.clip(0.1 + 3.9 * jax.random.uniform(key_of[5], (PARCELS,), jnp.float32) ** level_of(key_of[5], (PARCELS,), ((0, 256),), -0.2, 0.2), 0.1, 4.0)
    parcel_cell = draw_parcel_cell(jax.random.fold_in(key_of[8], 71), 0)
    parcel_count = draw_parcel_count(jax.random.fold_in(key_of[8], 71), 0)
    return dict(density=density, momentum=momentum, energy=energy, parcel_mass=parcel_mass, droplet_velocity=droplet_velocity, parcel_temp=parcel_temp, parcel_cell=parcel_cell, parcel_count=parcel_count)


ADIABATIC_INDEX = 1.4
KICK = 0.25
COURANT = 0.4
SHRINK = 0.5

def cell_sums(values, cell_ids, segments):
    return jax.ops.segment_sum(values, cell_ids, num_segments=segments)

def reference(density, momentum, energy, parcel_mass, droplet_velocity, parcel_temp, parcel_cell, parcel_count):
    row_index = jnp.arange(parcel_mass.shape[0], dtype=jnp.int32)
    device = row_index // P_DEV
    local_row = row_index % P_DEV
    live = local_row < parcel_count[device]
    boiled_off_amount = jnp.where(live, parcel_mass * jax.nn.sigmoid(2.0 * (parcel_temp - 2.0)), 0.0)
    specific_movement_budget = 0.5 * lax.optimization_barrier(jnp.sum(droplet_velocity * droplet_velocity, axis=0))
    sources = jnp.concatenate([boiled_off_amount[None], boiled_off_amount[None] * droplet_velocity, (boiled_off_amount * (parcel_temp + specific_movement_budget))[None]], axis=0)
    flat_cell = (parcel_cell[0] * NY + parcel_cell[1]) * NZ + parcel_cell[2]
    deposit = jax.vmap(lambda values: cell_sums(values, flat_cell, NX * NY * NZ))(sources).reshape(5, NX, NY, NZ)
    updated_fluid_density = density + deposit[0]
    energy_out = energy + deposit[4]
    lifted = momentum + deposit[1:4]
    normal_stress_field = (ADIABATIC_INDEX - 1.0) * energy_out
    padded = jnp.pad(normal_stress_field, 1)
    grad_x = 0.5 * (padded[2:, 1:-1, 1:-1] - padded[:-2, 1:-1, 1:-1])
    grad_y = 0.5 * (padded[1:-1, 2:, 1:-1] - padded[1:-1, :-2, 1:-1])
    grad_z = 0.5 * (padded[1:-1, 1:-1, 2:] - padded[1:-1, 1:-1, :-2])
    updated_fluid_impulse = lifted - KICK * jnp.stack([grad_x, grad_y, grad_z])
    ambient_stream_speed = updated_fluid_impulse / updated_fluid_density[None]
    acoustic_signal = lax.optimization_barrier(jnp.max(jnp.abs(ambient_stream_speed), axis=0)) + jnp.sqrt(ADIABATIC_INDEX * normal_stress_field / updated_fluid_density)
    time_step = COURANT / jnp.max(acoustic_signal)
    col_x = device // N_GY
    col_y = device % N_GY
    local_x = parcel_cell[0] - col_x * CX
    local_y = parcel_cell[1] - col_y * CY
    heading = jnp.where(local_x < 0, 0, jnp.where(local_x >= CX, 1, jnp.where(local_y < 0, 2, jnp.where(local_y >= CY, 3, 4))))
    heading = jnp.where(live, heading, 5).astype(jnp.int32)
    onehot = (heading[:, None] == jnp.arange(4, dtype=jnp.int32)[None]).astype(jnp.int32).reshape(DEVICES, P_DEV, 4)
    earlier = (jnp.cumsum(onehot, axis=1) - onehot).reshape(DEVICES * P_DEV, 4)
    rank = lax.optimization_barrier(jnp.sum(earlier * onehot.reshape(DEVICES * P_DEV, 4), axis=1))
    shift_table = jnp.array([-N_GY, N_GY, -1, 1, 0, 0], dtype=jnp.int32)
    bucket_table = jnp.array([1, 0, 3, 2, 0, 0], dtype=jnp.int32)
    target_dev = device + shift_table[heading]
    moving = jnp.where(heading < 4, target_dev * SLOTS + P_DEV + bucket_table[heading] * MOVE + rank, SLOTS * DEVICES)
    target = jnp.where(heading == 4, device * SLOTS + local_row, moving).astype(jnp.int32)
    carried_records = jnp.concatenate([(parcel_mass - SHRINK * boiled_off_amount)[None], droplet_velocity, parcel_temp[None], parcel_cell.astype(jnp.float32)], axis=0)
    table = jnp.zeros((8, SLOTS * DEVICES), carried_records.dtype).at[:, target].set(carried_records, mode='drop')
    moved_state = table[:5]
    moved_cell = table[5:].astype(jnp.int32)
    return (updated_fluid_density, updated_fluid_impulse, energy_out, moved_state, moved_cell, time_step)
```

```python
import functools

import jax
import jax.numpy as jnp
from jax import lax
from jax.experimental import pallas as pl
from jax.experimental.pallas import tpu as pltpu
from jax.sharding import PartitionSpec as P

ADIABATIC_INDEX = 1.4
KICK = 0.25
COURANT = 0.4
SHRINK = 0.5
MESH = pl.DeviceIdType.MESH
CHUNK = 1024
F32 = jnp.float32
BF16 = jnp.bfloat16
F8 = jnp.float8_e4m3fn
LIFT = 2048.0


def dot_nt(a, b):
    return lax.dot_general(a, b, (((1,), (1,)), ((), ())), preferred_element_type=F32)


def two_terms(x):
    high = x.astype(BF16)
    low = (x - high.astype(F32)).astype(BF16)
    return high, low


def one_hot_rows(row, count):
    lanes = row.shape[1]
    base = (
        jnp.broadcast_to(row, (16, lanes))
        - lax.broadcasted_iota(jnp.int32, (16, lanes), 0).astype(F32)
    ).astype(BF16)
    one, zero = jnp.ones((16, lanes), BF16), jnp.zeros((16, lanes), BF16)
    return jnp.concatenate(
        [jnp.where(base == 16.0 * k, one, zero) for k in range(count // 16)], axis=0
    )


def kernel(
    n_gx, n_gy, count_hbm, density_hbm, momentum_hbm, energy_hbm, mass_hbm, vel_hbm, temp_hbm, cell_hbm,
    rho_ref, imp_ref, en_ref, state_ref, moved_ref, step_ref,
    src_ref, pay_ref, col_ref, q_ref, r_ref, a0_ref, a1_ref, c0_ref, c1_ref, e0_ref, e1_ref, f0_ref, f1_ref,
    b0_ref, b1_ref, d0_ref, d1_ref, acc_ref, low_ref, small_ref,
    out_bucket, in_bucket, out_face, in_face, max_z, max_p,
    bucket_send, bucket_recv, face_send, face_recv, mz_send, mz_recv, mp_send, mp_recv,
    count_ref, density_ref, momentum_ref, energy_ref, mass_ref, vel_ref, temp_ref, cell_ref, load_sem,
):
    sources = (count_hbm, mass_hbm, temp_hbm, vel_hbm, cell_hbm, energy_hbm, density_hbm, momentum_hbm)
    places = (count_ref, mass_ref, temp_ref, vel_ref, cell_ref, energy_ref, density_ref, momentum_ref)
    loads = []
    for k in range(8):
        load = pltpu.make_async_copy(sources[k], places[k], load_sem.at[k])
        load.start()
        loads.append(load)
    gx, gy = lax.axis_index("gx"), lax.axis_index("gy")
    cx, cy, nz = density_ref.shape
    rows = mass_ref.shape[1]
    cap = rows // 16
    per = cap // 128

    half = n_gy // 2
    upper_half, plane = gy // half, lax.rem(gy, half)
    in_column, n_column = upper_half * n_gx + gx, 2 * n_gx

    def column_peer(k):
        place = lax.rem(in_column + k, n_column)
        return {"gx": lax.rem(place, n_gx), "gy": place // n_gx * half + plane}

    def plane_peer(k):
        return {"gy": upper_half * half + lax.rem(plane + k, half)}

    targets = (
        {"gx": lax.rem(gx + n_gx - 1, n_gx)},
        {"gx": lax.rem(gx + 1, n_gx)},
        {"gy": lax.rem(gy + n_gy - 1, n_gy)},
        {"gy": lax.rem(gy + 1, n_gy)},
    )
    landing = (1, 0, 3, 2)

    barrier = pltpu.get_barrier_semaphore()
    greeted = [column_peer(k) for k in range(1, n_column)] + [plane_peer(k) for k in range(1, half)] + list(targets[2:])
    for peer in greeted:
        pl.semaphore_signal(barrier, inc=1, device_id=peer, device_id_type=MESH)

    for load in loads[:5]:
        load.wait()
    mass, temp = mass_ref[...], temp_ref[...]
    live = lax.broadcasted_iota(jnp.int32, (1, rows), 1) < count_ref[0]
    evap = jnp.where(live, mass * jax.nn.sigmoid(2.0 * (temp - 2.0)), 0.0)
    vx, vy, vz = vel_ref[0:1, :], vel_ref[1:2, :], vel_ref[2:3, :]
    src_ref[0:1, :] = evap
    src_ref[1:2, :] = evap * vx
    src_ref[2:3, :] = evap * vy
    src_ref[3:4, :] = evap * vz
    src_ref[4:5, :] = evap * (temp + 0.5 * (vx * vx + vy * vy + vz * vz))
    pay_ref[0:1, :] = mass - SHRINK * evap
    pay_ref[1:4, :] = vel_ref[...]
    pay_ref[4:5, :] = temp
    pay_ref[5:8, :] = cell_ref[...].astype(F32)
    lx = cell_ref[0:1, :] - gx * cx
    ly = cell_ref[1:2, :] - gy * cy
    heading = jnp.where(
        lx < 0, 0, jnp.where(lx >= cx, 1, jnp.where(ly < 0, 2, jnp.where(ly >= cy, 3, 4)))
    )
    heading = jnp.where(live, heading, 5)
    stays = heading == 4
    col_ref[...] = jnp.where(stays, lx * cy + ly, -1000).astype(F32)
    state_ref[:, :rows] = jnp.where(stays, pay_ref[0:5, :], 0.0)
    moved_ref[:, :rows] = jnp.where(stays, cell_ref[...], 0)

    blocks = rows // 128
    marks = jnp.where(
        jnp.broadcast_to(heading, (8, rows)) == lax.broadcasted_iota(jnp.int32, (8, rows), 0), 1.0, 0.0
    )
    stacked = jnp.concatenate([marks[:, k * 128 : (k + 1) * 128] for k in range(blocks)], axis=0)
    i0 = lax.broadcasted_iota(jnp.int32, (128, 256), 0)
    i1 = lax.broadcasted_iota(jnp.int32, (128, 256), 1)
    upper = jnp.where((i0 < i1) | (i1 >= 128), 1.0, 0.0).astype(BF16)
    sums = jnp.dot(stacked.astype(BF16), upper, preferred_element_type=F32)
    carry = jnp.zeros((8, 128), F32)
    ranks = []
    for k in range(blocks):
        part = sums[k * 8 : (k + 1) * 8]
        mark = stacked[k * 8 : (k + 1) * 8]
        ranks.append(jnp.sum((part[:, :128] + carry) * mark, axis=0, keepdims=True))
        carry = carry + part[:, 128:]
    rank = jnp.concatenate(ranks, axis=1).astype(jnp.int32)
    q_ref[...] = jnp.where(heading < 4, heading * per + (rank >> 7), -1).astype(F32)
    r_ref[...] = (rank & 127).astype(F32)

    groups = 4 * per
    small_ref[...] = jnp.zeros_like(small_ref)

    def pack(c, carry):
        lanes = pl.ds(pl.multiple_of(c * CHUNK, CHUNK), CHUNK)
        high, low = two_terms(pay_ref[:, lanes])
        both = jnp.concatenate([high.astype(F32), low.astype(F32)], axis=0).astype(BF16)
        q = jnp.broadcast_to(q_ref[:, lanes], (16, CHUNK)).astype(BF16)
        zero = jnp.zeros((16, CHUNK), BF16)
        left = jnp.concatenate([jnp.where(q == float(k), both, zero) for k in range(groups)], axis=0)
        small_ref[...] += dot_nt(left, one_hot_rows(r_ref[:, lanes], 128))
        return carry

    lax.fori_loop(0, rows // CHUNK, pack, 0)
    for h in range(4):
        for j in range(per):
            k = (h * per + j) * 16
            out_bucket[h, :, j * 128 : (j + 1) * 128] = small_ref[k : k + 8, :] + small_ref[k + 8 : k + 16, :]

    def exchange(src, dst, send, recv):
        copies = []
        for h in range(4):
            copy = pltpu.make_async_remote_copy(
                src_ref=src.at[h], dst_ref=dst.at[landing[h]], send_sem=send.at[h],
                recv_sem=recv.at[landing[h]], device_id=targets[h], device_id_type=MESH,
            )
            copy.start()
            copies.append(copy)
        return copies

    cells = cx * cy
    chunks = rows // CHUNK
    acc_ref[...] = jnp.zeros_like(acc_ref)
    low_ref[...] = jnp.zeros_like(low_ref)

    def spread(lanes, values, a_ref, c_ref):
        base = (
            jnp.broadcast_to(col_ref[:, lanes], (16, CHUNK))
            - lax.broadcasted_iota(jnp.int32, (16, CHUNK), 0).astype(F32)
        ).astype(BF16)
        zero = jnp.zeros((16, CHUNK), BF16)
        hits = [base == 16.0 * k for k in range(cells // 16)]
        for n, v in enumerate(values):
            value = jnp.broadcast_to(src_ref[v : v + 1, lanes], (16, CHUNK))
            high = value.astype(BF16)
            low = ((value - high.astype(F32)) * LIFT).astype(BF16)
            for k in range(cells // 16):
                at = n * cells + k * 16
                a_ref[at : at + 16, :] = jnp.where(hits[k], high, zero)
            for k in range(0, cells // 16, 2):
                at = n * cells + k * 16
                pair = jnp.concatenate([jnp.where(hits[k], low, zero), jnp.where(hits[k + 1], low, zero)], axis=0)
                c_ref[at : at + 32, :] = pair.astype(F8)

    def chunk_of(c):
        return pl.ds(pl.multiple_of(c * CHUNK, CHUNK), CHUNK)

    e_rows = slice(4 * cells, 5 * cells)

    def build_energy(c, i, a_ref, c_ref, b_ref, d_ref):
        lanes, place = chunk_of(c), chunk_of(i)
        spread(lanes, (4,), a_ref, c_ref)
        depth = one_hot_rows(cell_ref[2:3, lanes].astype(F32), nz)
        b_ref[:, place] = depth
        d_ref[:, place] = depth.astype(F8)

    build_energy(0, 0, e0_ref, f0_ref, b0_ref, d0_ref)

    def two_energy(i, carry):
        place = chunk_of(i)
        acc_ref[e_rows, :] += dot_nt(e0_ref[...], b0_ref[:, place])
        low_ref[e_rows, :] += dot_nt(f0_ref[...], d0_ref[:, place])
        build_energy(2 * i + 1, i, e1_ref, f1_ref, b1_ref, d1_ref)
        acc_ref[e_rows, :] += dot_nt(e1_ref[...], b1_ref[:, place])
        low_ref[e_rows, :] += dot_nt(f1_ref[...], d1_ref[:, place])
        later = jnp.minimum(i + 1, chunks // 2 - 1)
        build_energy(2 * later, later, e0_ref, f0_ref, b0_ref, d0_ref)
        return carry

    lax.fori_loop(0, chunks // 2, two_energy, 0)

    pl.semaphore_wait(barrier, len(greeted))
    moves = exchange(out_bucket, in_bucket, bucket_send, bucket_recv)

    others = slice(0, 4 * cells)
    spread(chunk_of(0), (0, 1, 2, 3), a0_ref, c0_ref)

    def two_others(i, carry):
        place = chunk_of(i)
        acc_ref[others, :] += dot_nt(a0_ref[...], b0_ref[:, place])
        low_ref[others, :] += dot_nt(c0_ref[...], d0_ref[:, place])
        spread(chunk_of(2 * i + 1), (0, 1, 2, 3), a1_ref, c1_ref)
        acc_ref[others, :] += dot_nt(a1_ref[...], b1_ref[:, place])
        low_ref[others, :] += dot_nt(c1_ref[...], d1_ref[:, place])
        spread(chunk_of(jnp.minimum(2 * i + 2, chunks - 1)), (0, 1, 2, 3), a0_ref, c0_ref)
        return carry

    lax.fori_loop(0, chunks // 4, two_others, 0)

    for copy in moves:
        copy.wait_recv()
    for b in range(4):
        got = in_bucket[b]
        state_ref[:, rows + b * cap : rows + (b + 1) * cap] = got[0:5]
        moved_ref[:, rows + b * cap : rows + (b + 1) * cap] = got[5:8].astype(jnp.int32)
        warm = got[4:5]
        share = jax.nn.sigmoid(2.0 * (warm - 2.0))
        boiled = got[0:1] * share / (1.0 - SHRINK * share)
        speed = got[1:4]
        budget = 0.5 * jnp.sum(speed * speed, axis=0, keepdims=True)
        values = [boiled] + [boiled * got[k : k + 1] for k in (1, 2, 3)] + [boiled * (warm + budget)]
        if b < 2:
            along = got[6:7] - (gy * cy).astype(F32)
        else:
            along = got[5:6] - (gx * cx).astype(F32)
        hit = (
            jnp.broadcast_to(along, (16, cap))
            == lax.broadcasted_iota(jnp.int32, (16, cap), 0).astype(F32)
        )
        parts = []
        for value in values:
            wide = jnp.where(hit, jnp.broadcast_to(value, (16, cap)), 0.0)
            parts.append(two_terms(wide))
        left = jnp.concatenate([p[0] for p in parts] + [p[1] for p in parts], axis=0)
        depth = one_hot_rows(got[7:8], nz)
        sums = dot_nt(left, depth)
        sums = sums[0 : 5 * 16] + sums[5 * 16 : 10 * 16]
        for v in range(5):
            part = sums[v * 16 : (v + 1) * 16]
            if b < 2:
                at = v * cells + (0 if b == 0 else (cx - 1) * cy)
                acc_ref[at : at + cy, :] += part
            else:
                edge = 0 if b == 2 else cy - 1
                for x in range(cx):
                    at = v * cells + x * cy + edge
                    acc_ref[at : at + 1, :] += part[x : x + 1]

    def deposit(v):
        at = slice(v * cells, (v + 1) * cells)
        return (acc_ref[at, :] + low_ref[at, :] * (1.0 / LIFT)).reshape(cx, cy, nz)

    for load in loads[5:]:
        load.wait()
    energy = energy_ref[...] + deposit(4)
    en_ref[...] = energy
    out_face[0] = (ADIABATIC_INDEX - 1.0) * energy[0]
    out_face[1] = (ADIABATIC_INDEX - 1.0) * energy[cx - 1]
    for x in range(cx):
        out_face[2, x : x + 1, :] = (ADIABATIC_INDEX - 1.0) * energy[x, 0:1, :]
        out_face[3, x : x + 1, :] = (ADIABATIC_INDEX - 1.0) * energy[x, cy - 1 : cy, :]
    faces = exchange(out_face, in_face, face_send, face_recv)

    lax.fori_loop(chunks // 4, chunks // 2, two_others, 0)

    pressure = (ADIABATIC_INDEX - 1.0) * en_ref[...]
    density = density_ref[...] + deposit(0)
    rho_ref[...] = density
    lane = lax.broadcasted_iota(jnp.int32, (cx, cy, nz), 2)
    after = jnp.where(lane == nz - 1, 0.0, pltpu.roll(pressure, nz - 1, 2))
    before = jnp.where(lane == 0, 0.0, pltpu.roll(pressure, 1, 2))
    impulse_z = momentum_ref[2] + deposit(3) - KICK * (0.5 * (after - before))
    imp_ref[2] = impulse_z
    sound = jnp.sqrt(ADIABATIC_INDEX * pressure / density)
    for copy in faces:
        copy.wait_recv()
    low_x = jnp.where(gx > 0, in_face[0], 0.0)
    high_x = jnp.where(gx < n_gx - 1, in_face[1], 0.0)
    low_y = jnp.where(gy > 0, in_face[2], 0.0)
    high_y = jnp.where(gy < n_gy - 1, in_face[3], 0.0)
    after = jnp.concatenate([pressure[1:], high_x[None]], axis=0)
    before = jnp.concatenate([low_x[None], pressure[:-1]], axis=0)
    impulse_x = momentum_ref[0] + deposit(1) - KICK * (0.5 * (after - before))
    imp_ref[0] = impulse_x
    line = lax.broadcasted_iota(jnp.int32, (cx, cy, nz), 1)
    after = jnp.where(line == cy - 1, high_y[:, None, :], pltpu.roll(pressure, cy - 1, 1))
    before = jnp.where(line == 0, low_y[:, None, :], pltpu.roll(pressure, 1, 1))
    impulse_y = momentum_ref[1] + deposit(2) - KICK * (0.5 * (after - before))
    imp_ref[1] = impulse_y
    fastest = jnp.maximum(jnp.maximum(jnp.abs(impulse_x), jnp.abs(impulse_y)), jnp.abs(impulse_z))
    wave = fastest / density + sound

    def share_max(value, me, n, peer, slots, send, recv):
        slots[me] = value
        copies = []
        for k in range(1, n):
            copy = pltpu.make_async_remote_copy(
                src_ref=slots.at[me], dst_ref=slots.at[me], send_sem=send.at[k],
                recv_sem=recv.at[k], device_id=peer(k), device_id_type=MESH,
            )
            copy.start()
            copies.append(copy)
        for copy in copies:
            copy.wait_recv()
        return jnp.max(slots[...], axis=0), copies

    top = jnp.max(jnp.max(wave, axis=0), axis=0, keepdims=True)
    top = jnp.maximum(top[:, 0:128], top[:, 128:256])
    top, sent_p = share_max(top, plane, half, plane_peer, max_p, mp_send, mp_recv)
    top, sent_z = share_max(top, in_column, n_column, column_peer, max_z, mz_send, mz_recv)
    step_ref[...] = COURANT / jnp.broadcast_to(jnp.max(top), (1, 128))
    for copy in moves + faces + sent_p + sent_z:
        copy.wait_send()


def put_out(*refs):
    count = (len(refs) - 2) // 2
    step_ref, sem = refs[-2:]
    step_ref[0] = refs[count - 1][0, 0]
    copies = []
    for k in range(count):
        source = refs[k] if k < count - 1 else step_ref
        copy = pltpu.make_async_copy(source, refs[count + k], sem.at[k])
        copy.start()
        copies.append(copy)
    for copy in copies:
        copy.wait()


def on_device(n_gx, n_gy, density, momentum, energy, mass, velocity, temp, cell, count):
    rows = mass.shape[0]
    cap = rows // 16
    slots = rows + 4 * cap
    cx, cy, nz = density.shape
    vmem = pl.BlockSpec(memory_space=pltpu.VMEM)
    hbm = pl.BlockSpec(memory_space=pltpu.HBM)
    cells = cx * cy
    half = n_gy // 2
    dma = pltpu.SemaphoreType.DMA
    outs = pl.pallas_call(
        functools.partial(kernel, n_gx, n_gy),
        out_shape=(
            pltpu.VMEM(density.shape, F32),
            pltpu.VMEM(momentum.shape, F32),
            pltpu.VMEM(energy.shape, F32),
            pltpu.VMEM((5, slots), F32),
            pltpu.VMEM((3, slots), jnp.int32),
            pltpu.VMEM((1, 128), F32),
        ),
        in_specs=[hbm] * 8,
        out_specs=(vmem,) * 6,
        scratch_shapes=[
            pltpu.VMEM((8, rows), F32),
            pltpu.VMEM((8, rows), F32),
            pltpu.VMEM((1, rows), F32),
            pltpu.VMEM((1, rows), F32),
            pltpu.VMEM((1, rows), F32),
            pltpu.VMEM((4 * cells, CHUNK), BF16),
            pltpu.VMEM((4 * cells, CHUNK), BF16),
            pltpu.VMEM((4 * cells, CHUNK), F8),
            pltpu.VMEM((4 * cells, CHUNK), F8),
            pltpu.VMEM((cells, CHUNK), BF16),
            pltpu.VMEM((cells, CHUNK), BF16),
            pltpu.VMEM((cells, CHUNK), F8),
            pltpu.VMEM((cells, CHUNK), F8),
            pltpu.VMEM((nz, rows // 2), BF16),
            pltpu.VMEM((nz, rows // 2), BF16),
            pltpu.VMEM((nz, rows // 2), F8),
            pltpu.VMEM((nz, rows // 2), F8),
            pltpu.VMEM((5 * cells, nz), F32),
            pltpu.VMEM((5 * cells, nz), F32),
            pltpu.VMEM((4 * (cap // 128) * 16, 128), F32),
            pltpu.VMEM((4, 8, cap), F32),
            pltpu.VMEM((4, 8, cap), F32),
            pltpu.VMEM((4, cx, nz), F32),
            pltpu.VMEM((4, cx, nz), F32),
            pltpu.VMEM((2 * n_gx, 1, 128), F32),
            pltpu.VMEM((half, 1, 128), F32),
            dma((4,)),
            dma((4,)),
            dma((4,)),
            dma((4,)),
            dma((2 * n_gx,)),
            dma((2 * n_gx,)),
            dma((half,)),
            dma((half,)),
            pltpu.SMEM((1,), jnp.int32),
            pltpu.VMEM(density.shape, F32),
            pltpu.VMEM(momentum.shape, F32),
            pltpu.VMEM(energy.shape, F32),
            pltpu.VMEM((1, rows), F32),
            pltpu.VMEM(velocity.shape, F32),
            pltpu.VMEM((1, rows), F32),
            pltpu.VMEM(cell.shape, jnp.int32),
            dma((8,)),
        ],
        compiler_params=pltpu.CompilerParams(
            collective_id=0, has_side_effects=True, vmem_limit_bytes=64200000
        ),
        name="spray",
    )(count, density, momentum, energy, mass.reshape(1, rows), velocity, temp.reshape(1, rows), cell)
    final = pl.pallas_call(
        put_out,
        out_shape=tuple(pltpu.HBM(o.shape, o.dtype) for o in outs[:5]) + (pltpu.HBM((1,), F32),),
        in_specs=[vmem] * 6,
        out_specs=(hbm,) * 6,
        scratch_shapes=[pltpu.SMEM((1,), F32), dma((6,))],
        compiler_params=pltpu.CompilerParams(vmem_limit_bytes=8 * 1024 * 1024),
        name="put_out",
    )(*outs)
    return tuple(final[:5]) + (final[5].reshape(()),)


def solution(mesh):
    in_specs = (
        P("gx", "gy", None),
        P(None, "gx", "gy", None),
        P("gx", "gy", None),
        P(("gx", "gy")),
        P(None, ("gx", "gy")),
        P(("gx", "gy")),
        P(None, ("gx", "gy")),
        P(("gx", "gy")),
    )
    out_specs = (
        P("gx", "gy", None),
        P(None, "gx", "gy", None),
        P("gx", "gy", None),
        P(None, ("gx", "gy")),
        P(None, ("gx", "gy")),
        P(),
    )
    return jax.shard_map(
        functools.partial(on_device, mesh.shape["gx"], mesh.shape["gy"]),
        mesh=mesh, in_specs=in_specs, out_specs=out_specs, check_vma=False,
    )
```

```python
import functools

import jax
import jax.numpy as jnp
from jax import lax
from jax.experimental import pallas as pl
from jax.experimental.pallas import tpu as pltpu
from jax.sharding import PartitionSpec as P

ADIABATIC_INDEX = 1.4
KICK = 0.25
COURANT = 0.4
SHRINK = 0.5
MESH = pl.DeviceIdType.MESH
CHUNK = 1024
F32 = jnp.float32
BF16 = jnp.bfloat16
F8 = jnp.float8_e4m3fn
LIFT = 2048.0


def dot_nt(a, b):
    return lax.dot_general(a, b, (((1,), (1,)), ((), ())), preferred_element_type=F32)


def two_terms(x):
    high = x.astype(BF16)
    low = (x - high.astype(F32)).astype(BF16)
    return high, low


def one_hot_rows(row, count):
    lanes = row.shape[1]
    base = (
        jnp.broadcast_to(row, (16, lanes))
        - lax.broadcasted_iota(jnp.int32, (16, lanes), 0).astype(F32)
    ).astype(BF16)
    one, zero = jnp.ones((16, lanes), BF16), jnp.zeros((16, lanes), BF16)
    return jnp.concatenate(
        [jnp.where(base == 16.0 * k, one, zero) for k in range(count // 16)], axis=0
    )


def kernel(
    n_gx, n_gy, count_hbm, density_hbm, momentum_hbm, energy_hbm, mass_hbm, vel_hbm, temp_hbm, cell_hbm,
    rho_ref, imp_ref, en_ref, state_ref, moved_ref, step_ref,
    src_ref, pay_ref, col_ref, q_ref, r_ref, g0_ref, g1_ref, h0_ref, h1_ref, a0_ref, a1_ref, c0_ref, c1_ref, e0_ref, e1_ref, f0_ref, f1_ref,
    b0_ref, b1_ref, d0_ref, d1_ref, acc_ref, low_ref, small_ref,
    out_bucket, in_bucket, out_face, in_face, max_z, max_p,
    bucket_send, bucket_recv, face_send, face_recv, mz_send, mz_recv, mp_send, mp_recv,
    count_ref, density_ref, momentum_ref, energy_ref, mass_ref, vel_ref, temp_ref, cell_ref, load_sem,
):
    sources = (count_hbm, mass_hbm, temp_hbm, vel_hbm, cell_hbm, energy_hbm, density_hbm, momentum_hbm)
    places = (count_ref, mass_ref, temp_ref, vel_ref, cell_ref, energy_ref, density_ref, momentum_ref)
    loads = []
    for k in range(8):
        load = pltpu.make_async_copy(sources[k], places[k], load_sem.at[k])
        load.start()
        loads.append(load)
    gx, gy = lax.axis_index("gx"), lax.axis_index("gy")
    cx, cy, nz = density_ref.shape
    rows = mass_ref.shape[1]
    cap = rows // 16
    per = cap // 128

    half = n_gy // 2
    upper_half, plane = gy // half, lax.rem(gy, half)
    in_column, n_column = upper_half * n_gx + gx, 2 * n_gx

    def column_peer(k):
        place = lax.rem(in_column + k, n_column)
        return {"gx": lax.rem(place, n_gx), "gy": place // n_gx * half + plane}

    def plane_peer(k):
        return {"gy": upper_half * half + lax.rem(plane + k, half)}

    targets = (
        {"gx": lax.rem(gx + n_gx - 1, n_gx)},
        {"gx": lax.rem(gx + 1, n_gx)},
        {"gy": lax.rem(gy + n_gy - 1, n_gy)},
        {"gy": lax.rem(gy + 1, n_gy)},
    )
    landing = (1, 0, 3, 2)

    barrier = pltpu.get_barrier_semaphore()
    greeted = [column_peer(k) for k in range(1, n_column)] + [plane_peer(k) for k in range(1, half)] + list(targets[2:])
    for peer in greeted:
        pl.semaphore_signal(barrier, inc=1, device_id=peer, device_id_type=MESH)

    for load in loads[:5]:
        load.wait()
    mass, temp = mass_ref[...], temp_ref[...]
    live = lax.broadcasted_iota(jnp.int32, (1, rows), 1) < jnp.broadcast_to(count_ref[...], (1, rows))
    evap = jnp.where(live, mass * jax.nn.sigmoid(2.0 * (temp - 2.0)), 0.0)
    vx, vy, vz = vel_ref[0:1, :], vel_ref[1:2, :], vel_ref[2:3, :]
    src_ref[0:1, :] = evap
    src_ref[1:2, :] = evap * vx
    src_ref[2:3, :] = evap * vy
    src_ref[3:4, :] = evap * vz
    src_ref[4:5, :] = evap * (temp + 0.5 * (vx * vx + vy * vy + vz * vz))
    pay_ref[0:1, :] = mass - SHRINK * evap
    pay_ref[1:4, :] = vel_ref[...]
    pay_ref[4:5, :] = temp
    pay_ref[5:8, :] = cell_ref[...].astype(F32)
    lx = cell_ref[0:1, :] - gx * cx
    ly = cell_ref[1:2, :] - gy * cy
    heading = jnp.where(
        lx < 0, 0, jnp.where(lx >= cx, 1, jnp.where(ly < 0, 2, jnp.where(ly >= cy, 3, 4)))
    )
    heading = jnp.where(live, heading, 5)
    stays = heading == 4
    col_ref[...] = jnp.where(stays, lx * cy + ly, -1000).astype(F32)
    state_ref[:, :rows] = jnp.where(stays, pay_ref[0:5, :], 0.0)
    moved_ref[:, :rows] = jnp.where(stays, cell_ref[...], 0)

    blocks = rows // 128
    marks = jnp.where(
        jnp.broadcast_to(heading, (8, rows)) == lax.broadcasted_iota(jnp.int32, (8, rows), 0), 1.0, 0.0
    )
    stacked = jnp.concatenate([marks[:, k * 128 : (k + 1) * 128] for k in range(blocks)], axis=0)
    i0 = lax.broadcasted_iota(jnp.int32, (128, 256), 0)
    i1 = lax.broadcasted_iota(jnp.int32, (128, 256), 1)
    upper = jnp.where((i0 < i1) | (i1 >= 128), 1.0, 0.0).astype(BF16)
    sums = jnp.dot(stacked.astype(BF16), upper, preferred_element_type=F32)
    carry = jnp.zeros((8, 128), F32)
    ranks = []
    for k in range(blocks):
        part = sums[k * 8 : (k + 1) * 8]
        mark = stacked[k * 8 : (k + 1) * 8]
        ranks.append(jnp.sum((part[:, :128] + carry) * mark, axis=0, keepdims=True))
        carry = carry + part[:, 128:]
    rank = jnp.concatenate(ranks, axis=1).astype(jnp.int32)
    q_ref[...] = jnp.where(heading < 4, heading * per + (rank >> 7), -1).astype(F32)
    r_ref[...] = (rank & 127).astype(F32)

    inside = (gx > 0, gx < n_gx - 1, gy > 0, gy < n_gy - 1)

    def exchange(src, dst, send, recv):
        copies = []
        for h in range(4):
            copy = pltpu.make_async_remote_copy(
                src_ref=src.at[h], dst_ref=dst.at[landing[h]], send_sem=send.at[h],
                recv_sem=recv.at[landing[h]], device_id=targets[h], device_id_type=MESH,
            )
            pl.when(inside[h])(copy.start)
            copies.append(copy)
        return copies

    def wait_received(copies):
        for h in range(4):
            pl.when(inside[landing[h]])(copies[h].wait_recv)

    for b in range(4):
        @pl.when(jnp.logical_not(inside[b]))
        def _():
            in_bucket[b] = jnp.zeros(in_bucket.shape[1:], F32)

    cells = cx * cy
    chunks = rows // CHUNK
    groups = 4 * per
    small_ref[...] = jnp.zeros_like(small_ref)
    acc_ref[...] = jnp.zeros_like(acc_ref)
    low_ref[...] = jnp.zeros_like(low_ref)

    def spread(lanes, values, a_ref, c_ref):
        base = (
            jnp.broadcast_to(col_ref[:, lanes], (16, CHUNK))
            - lax.broadcasted_iota(jnp.int32, (16, CHUNK), 0).astype(F32)
        ).astype(BF16)
        zero = jnp.zeros((16, CHUNK), BF16)
        hits = [base == 16.0 * k for k in range(cells // 16)]
        for n, v in enumerate(values):
            value = jnp.broadcast_to(src_ref[v : v + 1, lanes], (16, CHUNK))
            high = value.astype(BF16)
            low = ((value - high.astype(F32)) * LIFT).astype(BF16)
            for k in range(cells // 16):
                at = n * cells + k * 16
                a_ref[at : at + 16, :] = jnp.where(hits[k], high, zero)
            for k in range(0, cells // 16, 2):
                at = n * cells + k * 16
                pair = jnp.concatenate([jnp.where(hits[k], low, zero), jnp.where(hits[k + 1], low, zero)], axis=0)
                c_ref[at : at + 32, :] = pair.astype(F8)

    def chunk_of(c):
        return pl.ds(pl.multiple_of(c * CHUNK, CHUNK), CHUNK)

    def build_pack(c, g_ref, h_ref):
        lanes = chunk_of(c)
        high, low = two_terms(pay_ref[:, lanes])
        both = jnp.concatenate([high.astype(F32), low.astype(F32)], axis=0).astype(BF16)
        q = jnp.broadcast_to(q_ref[:, lanes], (16, CHUNK)).astype(BF16)
        zero = jnp.zeros((16, CHUNK), BF16)
        for k in range(groups):
            g_ref[k * 16 : (k + 1) * 16, :] = jnp.where(q == float(k), both, zero)
        h_ref[...] = one_hot_rows(r_ref[:, lanes], 128)

    e_rows = slice(4 * cells, 5 * cells)

    def build_energy(c, i, a_ref, c_ref, b_ref, d_ref):
        lanes, place = chunk_of(c), chunk_of(i)
        spread(lanes, (4,), a_ref, c_ref)
        depth = one_hot_rows(cell_ref[2:3, lanes].astype(F32), nz)
        b_ref[:, place] = depth
        d_ref[:, place] = depth.astype(F8)

    build_energy(0, 0, e0_ref, f0_ref, b0_ref, d0_ref)
    build_pack(0, g0_ref, h0_ref)

    def two_energy(i, carry):
        place = chunk_of(i)
        acc_ref[e_rows, :] += dot_nt(e0_ref[...], b0_ref[:, place])
        low_ref[e_rows, :] += dot_nt(f0_ref[...], d0_ref[:, place])
        small_ref[...] += dot_nt(g0_ref[...], h0_ref[...])
        build_energy(2 * i + 1, i, e1_ref, f1_ref, b1_ref, d1_ref)
        build_pack(2 * i + 1, g1_ref, h1_ref)
        acc_ref[e_rows, :] += dot_nt(e1_ref[...], b1_ref[:, place])
        low_ref[e_rows, :] += dot_nt(f1_ref[...], d1_ref[:, place])
        small_ref[...] += dot_nt(g1_ref[...], h1_ref[...])
        later = jnp.minimum(i + 1, chunks // 2 - 1)
        build_energy(2 * later, later, e0_ref, f0_ref, b0_ref, d0_ref)
        build_pack(2 * later, g0_ref, h0_ref)
        return carry

    lax.fori_loop(0, chunks // 2, two_energy, 0)

    for h in range(4):
        for j in range(per):
            k = (h * per + j) * 16
            out_bucket[h, :, j * 128 : (j + 1) * 128] = small_ref[k : k + 8, :] + small_ref[k + 8 : k + 16, :]

    pl.semaphore_wait(barrier, len(greeted))
    moves = exchange(out_bucket, in_bucket, bucket_send, bucket_recv)

    others = slice(0, 4 * cells)
    spread(chunk_of(0), (0, 1, 2, 3), a0_ref, c0_ref)

    def two_others(i, carry):
        place = chunk_of(i)
        acc_ref[others, :] += dot_nt(a0_ref[...], b0_ref[:, place])
        low_ref[others, :] += dot_nt(c0_ref[...], d0_ref[:, place])
        spread(chunk_of(2 * i + 1), (0, 1, 2, 3), a1_ref, c1_ref)
        acc_ref[others, :] += dot_nt(a1_ref[...], b1_ref[:, place])
        low_ref[others, :] += dot_nt(c1_ref[...], d1_ref[:, place])
        spread(chunk_of(jnp.minimum(2 * i + 2, chunks - 1)), (0, 1, 2, 3), a0_ref, c0_ref)
        return carry

    lax.fori_loop(0, chunks // 4, two_others, 0)

    wait_received(moves)
    for b in range(4):
        got = in_bucket[b]
        state_ref[:, rows + b * cap : rows + (b + 1) * cap] = got[0:5]
        moved_ref[:, rows + b * cap : rows + (b + 1) * cap] = got[5:8].astype(jnp.int32)
        warm = got[4:5]
        share = jax.nn.sigmoid(2.0 * (warm - 2.0))
        boiled = got[0:1] * share / (1.0 - SHRINK * share)
        speed = got[1:4]
        budget = 0.5 * jnp.sum(speed * speed, axis=0, keepdims=True)
        values = [boiled] + [boiled * got[k : k + 1] for k in (1, 2, 3)] + [boiled * (warm + budget)]
        if b < 2:
            along = got[6:7] - (gy * cy).astype(F32)
        else:
            along = got[5:6] - (gx * cx).astype(F32)
        hit = (
            jnp.broadcast_to(along, (16, cap))
            == lax.broadcasted_iota(jnp.int32, (16, cap), 0).astype(F32)
        )
        parts = []
        for value in values:
            wide = jnp.where(hit, jnp.broadcast_to(value, (16, cap)), 0.0)
            parts.append(two_terms(wide))
        left = jnp.concatenate([p[0] for p in parts] + [p[1] for p in parts], axis=0)
        depth = one_hot_rows(got[7:8], nz)
        sums = dot_nt(left, depth)
        sums = sums[0 : 5 * 16] + sums[5 * 16 : 10 * 16]
        for v in range(5):
            part = sums[v * 16 : (v + 1) * 16]
            if b < 2:
                at = v * cells + (0 if b == 0 else (cx - 1) * cy)
                acc_ref[at : at + cy, :] += part
            else:
                edge = 0 if b == 2 else cy - 1
                for x in range(cx):
                    at = v * cells + x * cy + edge
                    acc_ref[at : at + 1, :] += part[x : x + 1]

    def deposit(v):
        at = slice(v * cells, (v + 1) * cells)
        return (acc_ref[at, :] + low_ref[at, :] * (1.0 / LIFT)).reshape(cx, cy, nz)

    for load in loads[5:]:
        load.wait()
    energy = energy_ref[...] + deposit(4)
    en_ref[...] = energy
    out_face[0] = (ADIABATIC_INDEX - 1.0) * energy[0]
    out_face[1] = (ADIABATIC_INDEX - 1.0) * energy[cx - 1]
    for x in range(cx):
        out_face[2, x : x + 1, :] = (ADIABATIC_INDEX - 1.0) * energy[x, 0:1, :]
        out_face[3, x : x + 1, :] = (ADIABATIC_INDEX - 1.0) * energy[x, cy - 1 : cy, :]
    faces = exchange(out_face, in_face, face_send, face_recv)

    lax.fori_loop(chunks // 4, chunks // 2, two_others, 0)

    pressure = (ADIABATIC_INDEX - 1.0) * en_ref[...]
    density = density_ref[...] + deposit(0)
    rho_ref[...] = density
    lane = lax.broadcasted_iota(jnp.int32, (cx, cy, nz), 2)
    after = jnp.where(lane == nz - 1, 0.0, pltpu.roll(pressure, nz - 1, 2))
    before = jnp.where(lane == 0, 0.0, pltpu.roll(pressure, 1, 2))
    impulse_z = momentum_ref[2] + deposit(3) - KICK * (0.5 * (after - before))
    imp_ref[2] = impulse_z
    sound = jnp.sqrt(ADIABATIC_INDEX * pressure / density)
    wait_received(faces)
    low_x = jnp.where(gx > 0, in_face[0], 0.0)
    high_x = jnp.where(gx < n_gx - 1, in_face[1], 0.0)
    low_y = jnp.where(gy > 0, in_face[2], 0.0)
    high_y = jnp.where(gy < n_gy - 1, in_face[3], 0.0)
    after = jnp.concatenate([pressure[1:], high_x[None]], axis=0)
    before = jnp.concatenate([low_x[None], pressure[:-1]], axis=0)
    impulse_x = momentum_ref[0] + deposit(1) - KICK * (0.5 * (after - before))
    imp_ref[0] = impulse_x
    line = lax.broadcasted_iota(jnp.int32, (cx, cy, nz), 1)
    after = jnp.where(line == cy - 1, high_y[:, None, :], pltpu.roll(pressure, cy - 1, 1))
    before = jnp.where(line == 0, low_y[:, None, :], pltpu.roll(pressure, 1, 1))
    impulse_y = momentum_ref[1] + deposit(2) - KICK * (0.5 * (after - before))
    imp_ref[1] = impulse_y
    fastest = jnp.maximum(jnp.maximum(jnp.abs(impulse_x), jnp.abs(impulse_y)), jnp.abs(impulse_z))
    wave = fastest / density + sound

    def share_max(value, me, n, peer, slots, send, recv):
        slots[me] = value
        copies = []
        for k in range(1, n):
            copy = pltpu.make_async_remote_copy(
                src_ref=slots.at[me], dst_ref=slots.at[me], send_sem=send.at[k],
                recv_sem=recv.at[k], device_id=peer(k), device_id_type=MESH,
            )
            copy.start()
            copies.append(copy)
        for copy in copies:
            copy.wait_recv()
        return jnp.max(slots[...], axis=0), copies

    top = jnp.max(jnp.max(wave, axis=0), axis=0, keepdims=True)
    top = jnp.maximum(top[:, 0:128], top[:, 128:256])
    top, sent_p = share_max(top, plane, half, plane_peer, max_p, mp_send, mp_recv)
    top, sent_z = share_max(top, in_column, n_column, column_peer, max_z, mz_send, mz_recv)
    step_ref[...] = COURANT / jnp.broadcast_to(jnp.max(top), (1, 128))
    for copies in (moves, faces):
        for h in range(4):
            pl.when(inside[h])(copies[h].wait_send)
    for copy in sent_p + sent_z:
        copy.wait_send()


def put_out(*refs):
    count = (len(refs) - 2) // 2
    step_ref, sem = refs[-2:]
    step_ref[0] = refs[count - 1][0, 0]
    copies = []
    for k in range(count):
        source = refs[k] if k < count - 1 else step_ref
        copy = pltpu.make_async_copy(source, refs[count + k], sem.at[k])
        copy.start()
        copies.append(copy)
    for copy in copies:
        copy.wait()


def on_device(n_gx, n_gy, density, momentum, energy, mass, velocity, temp, cell, count):
    rows = mass.shape[0]
    cap = rows // 16
    slots = rows + 4 * cap
    cx, cy, nz = density.shape
    vmem = pl.BlockSpec(memory_space=pltpu.VMEM)
    hbm = pl.BlockSpec(memory_space=pltpu.HBM)
    cells = cx * cy
    half = n_gy // 2
    dma = pltpu.SemaphoreType.DMA
    outs = pl.pallas_call(
        functools.partial(kernel, n_gx, n_gy),
        out_shape=(
            pltpu.VMEM(density.shape, F32),
            pltpu.VMEM(momentum.shape, F32),
            pltpu.VMEM(energy.shape, F32),
            pltpu.VMEM((5, slots), F32),
            pltpu.VMEM((3, slots), jnp.int32),
            pltpu.VMEM((1, 128), F32),
        ),
        in_specs=[hbm] * 8,
        out_specs=(vmem,) * 6,
        scratch_shapes=[
            pltpu.VMEM((8, rows), F32),
            pltpu.VMEM((8, rows), F32),
            pltpu.VMEM((1, rows), F32),
            pltpu.VMEM((1, rows), F32),
            pltpu.VMEM((1, rows), F32),
            pltpu.VMEM((4 * (cap // 128) * 16, CHUNK), BF16),
            pltpu.VMEM((4 * (cap // 128) * 16, CHUNK), BF16),
            pltpu.VMEM((128, CHUNK), BF16),
            pltpu.VMEM((128, CHUNK), BF16),
            pltpu.VMEM((4 * cells, CHUNK), BF16),
            pltpu.VMEM((4 * cells, CHUNK), BF16),
            pltpu.VMEM((4 * cells, CHUNK), F8),
            pltpu.VMEM((4 * cells, CHUNK), F8),
            pltpu.VMEM((cells, CHUNK), BF16),
            pltpu.VMEM((cells, CHUNK), BF16),
            pltpu.VMEM((cells, CHUNK), F8),
            pltpu.VMEM((cells, CHUNK), F8),
            pltpu.VMEM((nz, rows // 2), BF16),
            pltpu.VMEM((nz, rows // 2), BF16),
            pltpu.VMEM((nz, rows // 2), F8),
            pltpu.VMEM((nz, rows // 2), F8),
            pltpu.VMEM((5 * cells, nz), F32),
            pltpu.VMEM((5 * cells, nz), F32),
            pltpu.VMEM((4 * (cap // 128) * 16, 128), F32),
            pltpu.VMEM((4, 8, cap), F32),
            pltpu.VMEM((4, 8, cap), F32),
            pltpu.VMEM((4, cx, nz), F32),
            pltpu.VMEM((4, cx, nz), F32),
            pltpu.VMEM((2 * n_gx, 1, 128), F32),
            pltpu.VMEM((half, 1, 128), F32),
            dma((4,)),
            dma((4,)),
            dma((4,)),
            dma((4,)),
            dma((2 * n_gx,)),
            dma((2 * n_gx,)),
            dma((half,)),
            dma((half,)),
            pltpu.VMEM((1, 1), jnp.int32),
            pltpu.VMEM(density.shape, F32),
            pltpu.VMEM(momentum.shape, F32),
            pltpu.VMEM(energy.shape, F32),
            pltpu.VMEM((1, rows), F32),
            pltpu.VMEM(velocity.shape, F32),
            pltpu.VMEM((1, rows), F32),
            pltpu.VMEM(cell.shape, jnp.int32),
            dma((8,)),
        ],
        compiler_params=pltpu.CompilerParams(
            collective_id=0, has_side_effects=True, vmem_limit_bytes=64200000
        ),
        name="spray",
    )(count.reshape(1, 1), density, momentum, energy, mass.reshape(1, rows), velocity, temp.reshape(1, rows), cell)
    final = pl.pallas_call(
        put_out,
        out_shape=tuple(pltpu.HBM(o.shape, o.dtype) for o in outs[:5]) + (pltpu.HBM((1,), F32),),
        in_specs=[vmem] * 6,
        out_specs=(hbm,) * 6,
        scratch_shapes=[pltpu.SMEM((1,), F32), dma((6,))],
        compiler_params=pltpu.CompilerParams(vmem_limit_bytes=8 * 1024 * 1024),
        name="put_out",
    )(*outs)
    return tuple(final[:5]) + (final[5].reshape(()),)


def solution(mesh):
    in_specs = (
        P("gx", "gy", None),
        P(None, "gx", "gy", None),
        P("gx", "gy", None),
        P(("gx", "gy")),
        P(None, ("gx", "gy")),
        P(("gx", "gy")),
        P(None, ("gx", "gy")),
        P(("gx", "gy")),
    )
    out_specs = (
        P("gx", "gy", None),
        P(None, "gx", "gy", None),
        P("gx", "gy", None),
        P(None, ("gx", "gy")),
        P(None, ("gx", "gy")),
        P(),
    )
    return jax.shard_map(
        functools.partial(on_device, mesh.shape["gx"], mesh.shape["gy"]),
        mesh=mesh, in_specs=in_specs, out_specs=out_specs, check_vma=False,
    )
```

```python
import functools

import jax
import jax.numpy as jnp
from jax import lax
from jax.experimental import pallas as pl
from jax.experimental.pallas import tpu as pltpu
from jax.sharding import PartitionSpec as P

ADIABATIC_INDEX = 1.4
KICK = 0.25
COURANT = 0.4
SHRINK = 0.5
MESH = pl.DeviceIdType.MESH
CHUNK = 1024
F32 = jnp.float32
BF16 = jnp.bfloat16
F8 = jnp.float8_e4m3fn
LIFT = 2048.0
SEND_AT = 2


def dot_nt(a, b):
    return lax.dot_general(a, b, (((1,), (1,)), ((), ())), preferred_element_type=F32)


def two_terms(x):
    high = x.astype(BF16)
    low = (x - high.astype(F32)).astype(BF16)
    return high, low


def one_hot_rows(row, count):
    lanes = row.shape[1]
    base = (
        jnp.broadcast_to(row, (16, lanes))
        - lax.broadcasted_iota(jnp.int32, (16, lanes), 0).astype(F32)
    ).astype(BF16)
    one, zero = jnp.ones((16, lanes), BF16), jnp.zeros((16, lanes), BF16)
    return jnp.concatenate(
        [jnp.where(base == 16.0 * k, one, zero) for k in range(count // 16)], axis=0
    )


def kernel(
    n_gx, n_gy, count_hbm, density_hbm, momentum_hbm, energy_hbm, mass_hbm, vel_hbm, temp_hbm, cell_hbm,
    rho_ref, imp_ref, en_ref, state_ref, moved_ref, step_ref,
    src_ref, pay_ref, col_ref, q_ref, r_ref, g0_ref, g1_ref, h0_ref, h1_ref, a0_ref, a1_ref, c0_ref, c1_ref, e0_ref, e1_ref, f0_ref, f1_ref,
    b0_ref, b1_ref, d0_ref, d1_ref, acc_ref, low_ref, small_ref,
    out_bucket, in_bucket, out_face, in_face, own_ref, max_z, max_p,
    bucket_send, bucket_recv, face_send, face_recv, mz_send, mz_recv, mp_send, mp_recv,
    count_ref, density_ref, momentum_ref, energy_ref, mass_ref, vel_ref, temp_ref, cell_ref, load_sem,
):
    sources = (count_hbm, mass_hbm, temp_hbm, vel_hbm, cell_hbm, energy_hbm, density_hbm, momentum_hbm)
    places = (count_ref, mass_ref, temp_ref, vel_ref, cell_ref, energy_ref, density_ref, momentum_ref)
    loads = []
    for k in range(8):
        load = pltpu.make_async_copy(sources[k], places[k], load_sem.at[k])
        load.start()
        loads.append(load)
    gx, gy = lax.axis_index("gx"), lax.axis_index("gy")
    cx, cy, nz = density_ref.shape
    rows = mass_ref.shape[1]
    cap = rows // 16
    per = cap // 128

    half = n_gy // 2
    upper_half, plane = gy // half, lax.rem(gy, half)
    in_column, n_column = upper_half * n_gx + gx, 2 * n_gx

    def column_peer(k):
        place = lax.rem(in_column + k, n_column)
        return {"gx": lax.rem(place, n_gx), "gy": place // n_gx * half + plane}

    def plane_peer(k):
        return {"gy": upper_half * half + lax.rem(plane + k, half)}

    targets = (
        {"gx": lax.rem(gx + n_gx - 1, n_gx)},
        {"gx": lax.rem(gx + 1, n_gx)},
        {"gy": lax.rem(gy + n_gy - 1, n_gy)},
        {"gy": lax.rem(gy + 1, n_gy)},
    )
    landing = (1, 0, 3, 2)

    barrier = pltpu.get_barrier_semaphore()
    greeted = [column_peer(k) for k in range(1, n_column)] + [plane_peer(k) for k in range(1, half)] + list(targets[2:])
    for peer in greeted:
        pl.semaphore_signal(barrier, inc=1, device_id=peer, device_id_type=MESH)

    for zeroed in (small_ref, acc_ref, low_ref):
        zeroed[...] = jnp.zeros_like(zeroed)
    for load in loads[:5]:
        load.wait()
    mass, temp = mass_ref[...], temp_ref[...]
    live = lax.broadcasted_iota(jnp.int32, (1, rows), 1) < jnp.broadcast_to(count_ref[...], (1, rows))
    evap = jnp.where(live, mass * jax.nn.sigmoid(2.0 * (temp - 2.0)), 0.0)
    vx, vy, vz = vel_ref[0:1, :], vel_ref[1:2, :], vel_ref[2:3, :]
    src_ref[0:1, :] = evap
    src_ref[1:2, :] = evap * vx
    src_ref[2:3, :] = evap * vy
    src_ref[3:4, :] = evap * vz
    src_ref[4:5, :] = evap * (temp + 0.5 * (vx * vx + vy * vy + vz * vz))
    pay_ref[0:1, :] = mass - SHRINK * evap
    pay_ref[1:4, :] = vel_ref[...]
    pay_ref[4:5, :] = temp
    pay_ref[5:8, :] = cell_ref[...].astype(F32)
    lx = cell_ref[0:1, :] - gx * cx
    ly = cell_ref[1:2, :] - gy * cy
    heading = jnp.where(
        lx < 0, 0, jnp.where(lx >= cx, 1, jnp.where(ly < 0, 2, jnp.where(ly >= cy, 3, 4)))
    )
    heading = jnp.where(live, heading, 5)
    stays = heading == 4
    col_ref[...] = jnp.where(stays, lx * cy + ly, -1000).astype(F32)
    state_ref[:, :rows] = jnp.where(stays, pay_ref[0:5, :], 0.0)
    moved_ref[:, :rows] = jnp.where(stays, cell_ref[...], 0)

    blocks = rows // 128
    marks = jnp.where(
        jnp.broadcast_to(heading, (8, rows)) == lax.broadcasted_iota(jnp.int32, (8, rows), 0), 1.0, 0.0
    )
    stacked = jnp.concatenate([marks[:, k * 128 : (k + 1) * 128] for k in range(blocks)], axis=0)
    i0 = lax.broadcasted_iota(jnp.int32, (128, 256), 0)
    i1 = lax.broadcasted_iota(jnp.int32, (128, 256), 1)
    upper = jnp.where((i0 < i1) | (i1 >= 128), 1.0, 0.0).astype(BF16)
    sums = jnp.dot(stacked.astype(BF16), upper, preferred_element_type=F32)
    carry = jnp.zeros((8, 128), F32)
    ranks = []
    for k in range(blocks):
        part = sums[k * 8 : (k + 1) * 8]
        mark = stacked[k * 8 : (k + 1) * 8]
        ranks.append(jnp.sum((part[:, :128] + carry) * mark, axis=0, keepdims=True))
        carry = carry + part[:, 128:]
    rank = jnp.concatenate(ranks, axis=1).astype(jnp.int32)
    q_ref[...] = jnp.where(heading < 4, heading * per + (rank >> 7), -1).astype(F32)
    r_ref[...] = (rank & 127).astype(F32)

    inside = (gx > 0, gx < n_gx - 1, gy > 0, gy < n_gy - 1)

    def exchange(src, dst, send, recv):
        copies = []
        for h in range(4):
            copy = pltpu.make_async_remote_copy(
                src_ref=src.at[h], dst_ref=dst.at[landing[h]], send_sem=send.at[h],
                recv_sem=recv.at[landing[h]], device_id=targets[h], device_id_type=MESH,
            )
            copies.append(copy)
        return copies

    def send(copies, which):
        for h in which:
            pl.when(inside[h])(copies[h].start)

    def wait_received(copies, which):
        for h in which:
            pl.when(inside[landing[h]])(copies[h].wait_recv)

    for b in range(4):
        @pl.when(jnp.logical_not(inside[b]))
        def _():
            in_bucket[b] = jnp.zeros(in_bucket.shape[1:], F32)

    cells = cx * cy
    chunks = rows // CHUNK
    groups = 4 * per

    def spread(lanes, values, a_ref, c_ref):
        base = (
            jnp.broadcast_to(col_ref[:, lanes], (16, CHUNK))
            - lax.broadcasted_iota(jnp.int32, (16, CHUNK), 0).astype(F32)
        ).astype(BF16)
        zero = jnp.zeros((16, CHUNK), BF16)
        hits = [base == 16.0 * k for k in range(cells // 16)]
        for n, v in enumerate(values):
            value = jnp.broadcast_to(src_ref[v : v + 1, lanes], (16, CHUNK))
            high = value.astype(BF16)
            low = ((value - high.astype(F32)) * LIFT).astype(BF16)
            for k in range(cells // 16):
                at = n * cells + k * 16
                a_ref[at : at + 16, :] = jnp.where(hits[k], high, zero)
            for k in range(0, cells // 16, 2):
                at = n * cells + k * 16
                pair = jnp.concatenate([jnp.where(hits[k], low, zero), jnp.where(hits[k + 1], low, zero)], axis=0)
                c_ref[at : at + 32, :] = pair.astype(F8)

    def chunk_of(c):
        if isinstance(c, int):
            return slice(c * CHUNK, (c + 1) * CHUNK)
        return pl.ds(pl.multiple_of(c * CHUNK, CHUNK), CHUNK)

    def build_pack(c, g_ref, h_ref):
        lanes = chunk_of(c)
        high, low = two_terms(pay_ref[:, lanes])
        both = jnp.concatenate([high.astype(F32), low.astype(F32)], axis=0).astype(BF16)
        q = jnp.broadcast_to(q_ref[:, lanes], (16, CHUNK)).astype(BF16)
        zero = jnp.zeros((16, CHUNK), BF16)
        for k in range(groups):
            g_ref[k * 16 : (k + 1) * 16, :] = jnp.where(q == float(k), both, zero)
        h_ref[...] = one_hot_rows(r_ref[:, lanes], 128)

    build_pack(0, g0_ref, h0_ref)

    def two_packs(i, carry):
        small_ref[...] += dot_nt(g0_ref[...], h0_ref[...])
        build_pack(2 * i + 1, g1_ref, h1_ref)
        small_ref[...] += dot_nt(g1_ref[...], h1_ref[...])
        build_pack(jnp.minimum(2 * i + 2, chunks - 1), g0_ref, h0_ref)
        return carry

    lax.fori_loop(0, chunks // 2, two_packs, 0)
    for h in range(4):
        for j in range(per):
            k = (h * per + j) * 16
            out_bucket[h, :, j * 128 : (j + 1) * 128] = small_ref[k : k + 8, :] + small_ref[k + 8 : k + 16, :]

    moves = exchange(out_bucket, in_bucket, bucket_send, bucket_recv)
    faces = exchange(out_face, in_face, face_send, face_recv)

    e_rows = slice(4 * cells, 5 * cells)

    def build_energy(c, i, a_ref, c_ref, b_ref, d_ref):
        lanes, place = chunk_of(c), chunk_of(i)
        spread(lanes, (4,), a_ref, c_ref)
        depth = one_hot_rows(cell_ref[2:3, lanes].astype(F32), nz)
        b_ref[:, place] = depth
        d_ref[:, place] = depth.astype(F8)

    build_energy(0, 0, e0_ref, f0_ref, b0_ref, d0_ref)

    def send_moves():
        pl.semaphore_wait(barrier, len(greeted))
        send(moves, (2, 3, 0, 1))

    def two_energy(i, carry):
        pl.when(i == SEND_AT)(send_moves)
        place = chunk_of(i)
        acc_ref[e_rows, :] += dot_nt(e0_ref[...], b0_ref[:, place])
        low_ref[e_rows, :] += dot_nt(f0_ref[...], d0_ref[:, place])
        build_energy(2 * i + 1, i, e1_ref, f1_ref, b1_ref, d1_ref)
        acc_ref[e_rows, :] += dot_nt(e1_ref[...], b1_ref[:, place])
        low_ref[e_rows, :] += dot_nt(f1_ref[...], d1_ref[:, place])
        later = jnp.minimum(i + 1, chunks // 2 - 1)
        build_energy(2 * later, later, e0_ref, f0_ref, b0_ref, d0_ref)
        return carry

    lax.fori_loop(0, chunks // 2, two_energy, 0)

    def sums_of(got, b, with_all):
        warm = got[4:5]
        share = jax.nn.sigmoid(2.0 * (warm - 2.0))
        boiled = got[0:1] * share / (1.0 - SHRINK * share)
        speed = got[1:4]
        budget = 0.5 * jnp.sum(speed * speed, axis=0, keepdims=True)
        values = [boiled * (warm + budget)]
        if with_all:
            values = [boiled] + [boiled * got[k : k + 1] for k in (1, 2, 3)] + values
        if b < 2:
            along = got[6:7] - (gy * cy).astype(F32)
        else:
            along = got[5:6] - (gx * cx).astype(F32)
        hit = (
            jnp.broadcast_to(along, (16, cap))
            == lax.broadcasted_iota(jnp.int32, (16, cap), 0).astype(F32)
        )
        parts = []
        for value in values:
            wide = jnp.where(hit, jnp.broadcast_to(value, (16, cap)), 0.0)
            parts.append(two_terms(wide))
        left = jnp.concatenate([p[0] for p in parts] + [p[1] for p in parts], axis=0)
        sums = dot_nt(left, one_hot_rows(got[7:8], nz))
        n = len(values) * 16
        return sums[0:n] + sums[n : 2 * n]

    def receive(b):
        got = in_bucket[b]
        state_ref[:, rows + b * cap : rows + (b + 1) * cap] = got[0:5]
        moved_ref[:, rows + b * cap : rows + (b + 1) * cap] = got[5:8].astype(jnp.int32)
        sums = sums_of(got, b, True)
        for v in range(5):
            part = sums[v * 16 : (v + 1) * 16]
            if b < 2:
                at = v * cells + (0 if b == 0 else (cx - 1) * cy)
                acc_ref[at : at + cy, :] += part
            else:
                edge = 0 if b == 2 else cy - 1
                for x in range(cx):
                    at = v * cells + x * cy + edge
                    acc_ref[at : at + 1, :] += part[x : x + 1]

    def deposit(v):
        at = slice(v * cells, (v + 1) * cells)
        return (acc_ref[at, :] + low_ref[at, :] * (1.0 / LIFT)).reshape(cx, cy, nz)

    def receive_x():
        wait_received(moves, (0, 1))
        receive(0)
        receive(1)
        for load in loads[5:]:
            load.wait()
        energy = energy_ref[...] + deposit(4)
        for x in range(cx):
            out_face[2, x : x + 1, :] = (ADIABATIC_INDEX - 1.0) * energy[x, 0:1, :]
            out_face[3, x : x + 1, :] = (ADIABATIC_INDEX - 1.0) * energy[x, cy - 1 : cy, :]
        send(faces, (2, 3))

    def receive_y():
        wait_received(moves, (2, 3))
        receive(2)
        receive(3)
        for h in (2, 3):
            own_ref[h - 2] = (ADIABATIC_INDEX - 1.0) * sums_of(out_bucket[h], h, False)
        energy = energy_ref[...] + deposit(4)
        en_ref[...] = energy
        out_face[0] = (ADIABATIC_INDEX - 1.0) * energy[0]
        out_face[1] = (ADIABATIC_INDEX - 1.0) * energy[cx - 1]
        send(faces, (0, 1))

    others = slice(0, 4 * cells)
    spread(chunk_of(0), (0, 1, 2, 3), a0_ref, c0_ref)

    def two_others(i, carry):
        pl.when(i == 1)(receive_x)
        pl.when(i == 2)(receive_y)
        place = chunk_of(i)
        acc_ref[others, :] += dot_nt(a0_ref[...], b0_ref[:, place])
        low_ref[others, :] += dot_nt(c0_ref[...], d0_ref[:, place])
        spread(chunk_of(2 * i + 1), (0, 1, 2, 3), a1_ref, c1_ref)
        acc_ref[others, :] += dot_nt(a1_ref[...], b1_ref[:, place])
        low_ref[others, :] += dot_nt(c1_ref[...], d1_ref[:, place])
        spread(chunk_of(jnp.minimum(2 * i + 2, chunks - 1)), (0, 1, 2, 3), a0_ref, c0_ref)
        return carry

    lax.fori_loop(0, chunks // 2, two_others, 0)

    pressure = (ADIABATIC_INDEX - 1.0) * en_ref[...]
    density = density_ref[...] + deposit(0)
    rho_ref[...] = density
    lane = lax.broadcasted_iota(jnp.int32, (cx, cy, nz), 2)
    after = jnp.where(lane == nz - 1, 0.0, pltpu.roll(pressure, nz - 1, 2))
    before = jnp.where(lane == 0, 0.0, pltpu.roll(pressure, 1, 2))
    impulse_z = momentum_ref[2] + deposit(3) - KICK * (0.5 * (after - before))
    imp_ref[2] = impulse_z
    sound = jnp.sqrt(ADIABATIC_INDEX * pressure / density)
    wait_received(faces, range(4))
    low_x = jnp.where(gx > 0, in_face[0], 0.0)
    high_x = jnp.where(gx < n_gx - 1, in_face[1], 0.0)
    low_y = jnp.where(gy > 0, in_face[2] + own_ref[0], 0.0)
    high_y = jnp.where(gy < n_gy - 1, in_face[3] + own_ref[1], 0.0)
    after = jnp.concatenate([pressure[1:], high_x[None]], axis=0)
    before = jnp.concatenate([low_x[None], pressure[:-1]], axis=0)
    impulse_x = momentum_ref[0] + deposit(1) - KICK * (0.5 * (after - before))
    imp_ref[0] = impulse_x
    line = lax.broadcasted_iota(jnp.int32, (cx, cy, nz), 1)
    after = jnp.where(line == cy - 1, high_y[:, None, :], pltpu.roll(pressure, cy - 1, 1))
    before = jnp.where(line == 0, low_y[:, None, :], pltpu.roll(pressure, 1, 1))
    impulse_y = momentum_ref[1] + deposit(2) - KICK * (0.5 * (after - before))
    imp_ref[1] = impulse_y
    fastest = jnp.maximum(jnp.maximum(jnp.abs(impulse_x), jnp.abs(impulse_y)), jnp.abs(impulse_z))
    wave = fastest / density + sound

    def share_max(value, me, n, peer, slots, send, recv):
        slots[me] = value
        copies = []
        for k in range(1, n):
            copy = pltpu.make_async_remote_copy(
                src_ref=slots.at[me], dst_ref=slots.at[me], send_sem=send.at[k],
                recv_sem=recv.at[k], device_id=peer(k), device_id_type=MESH,
            )
            copy.start()
            copies.append(copy)
        for copy in copies:
            copy.wait_recv()
        return jnp.max(slots[...], axis=0), copies

    top = jnp.max(jnp.max(wave, axis=0), axis=0, keepdims=True)
    top = jnp.maximum(top[:, 0:128], top[:, 128:256])
    top, sent_p = share_max(top, plane, half, plane_peer, max_p, mp_send, mp_recv)
    top, sent_z = share_max(top, in_column, n_column, column_peer, max_z, mz_send, mz_recv)
    step_ref[...] = COURANT / jnp.broadcast_to(jnp.max(top), (1, 128))
    for copies in (moves, faces):
        for h in range(4):
            pl.when(inside[h])(copies[h].wait_send)
    for copy in sent_p + sent_z:
        copy.wait_send()


def put_out(*refs):
    count = (len(refs) - 2) // 2
    step_ref, sem = refs[-2:]
    step_ref[0] = refs[count - 1][0, 0]
    copies = []
    for k in range(count):
        source = refs[k] if k < count - 1 else step_ref
        copy = pltpu.make_async_copy(source, refs[count + k], sem.at[k])
        copy.start()
        copies.append(copy)
    for copy in copies:
        copy.wait()


def on_device(n_gx, n_gy, density, momentum, energy, mass, velocity, temp, cell, count):
    rows = mass.shape[0]
    cap = rows // 16
    slots = rows + 4 * cap
    cx, cy, nz = density.shape
    vmem = pl.BlockSpec(memory_space=pltpu.VMEM)
    hbm = pl.BlockSpec(memory_space=pltpu.HBM)
    cells = cx * cy
    half = n_gy // 2
    dma = pltpu.SemaphoreType.DMA
    outs = pl.pallas_call(
        functools.partial(kernel, n_gx, n_gy),
        out_shape=(
            pltpu.VMEM(density.shape, F32),
            pltpu.VMEM(momentum.shape, F32),
            pltpu.VMEM(energy.shape, F32),
            pltpu.VMEM((5, slots), F32),
            pltpu.VMEM((3, slots), jnp.int32),
            pltpu.VMEM((1, 128), F32),
        ),
        in_specs=[hbm] * 8,
        out_specs=(vmem,) * 6,
        scratch_shapes=[
            pltpu.VMEM((8, rows), F32),
            pltpu.VMEM((8, rows), F32),
            pltpu.VMEM((1, rows), F32),
            pltpu.VMEM((1, rows), F32),
            pltpu.VMEM((1, rows), F32),
            pltpu.VMEM((4 * (cap // 128) * 16, CHUNK), BF16),
            pltpu.VMEM((4 * (cap // 128) * 16, CHUNK), BF16),
            pltpu.VMEM((128, CHUNK), BF16),
            pltpu.VMEM((128, CHUNK), BF16),
            pltpu.VMEM((4 * cells, CHUNK), BF16),
            pltpu.VMEM((4 * cells, CHUNK), BF16),
            pltpu.VMEM((4 * cells, CHUNK), F8),
            pltpu.VMEM((4 * cells, CHUNK), F8),
            pltpu.VMEM((cells, CHUNK), BF16),
            pltpu.VMEM((cells, CHUNK), BF16),
            pltpu.VMEM((cells, CHUNK), F8),
            pltpu.VMEM((cells, CHUNK), F8),
            pltpu.VMEM((nz, rows // 2), BF16),
            pltpu.VMEM((nz, rows // 2), BF16),
            pltpu.VMEM((nz, rows // 2), F8),
            pltpu.VMEM((nz, rows // 2), F8),
            pltpu.VMEM((5 * cells, nz), F32),
            pltpu.VMEM((5 * cells, nz), F32),
            pltpu.VMEM((4 * (cap // 128) * 16, 128), F32),
            pltpu.VMEM((4, 8, cap), F32),
            pltpu.VMEM((4, 8, cap), F32),
            pltpu.VMEM((4, cx, nz), F32),
            pltpu.VMEM((4, cx, nz), F32),
            pltpu.VMEM((2, cx, nz), F32),
            pltpu.VMEM((2 * n_gx, 1, 128), F32),
            pltpu.VMEM((half, 1, 128), F32),
            dma((4,)),
            dma((4,)),
            dma((4,)),
            dma((4,)),
            dma((2 * n_gx,)),
            dma((2 * n_gx,)),
            dma((half,)),
            dma((half,)),
            pltpu.VMEM((1, 1), jnp.int32),
            pltpu.VMEM(density.shape, F32),
            pltpu.VMEM(momentum.shape, F32),
            pltpu.VMEM(energy.shape, F32),
            pltpu.VMEM((1, rows), F32),
            pltpu.VMEM(velocity.shape, F32),
            pltpu.VMEM((1, rows), F32),
            pltpu.VMEM(cell.shape, jnp.int32),
            dma((8,)),
        ],
        compiler_params=pltpu.CompilerParams(
            collective_id=0, has_side_effects=True, vmem_limit_bytes=64200000
        ),
        name="spray",
    )(count.reshape(1, 1), density, momentum, energy, mass.reshape(1, rows), velocity, temp.reshape(1, rows), cell)
    final = pl.pallas_call(
        put_out,
        out_shape=tuple(pltpu.HBM(o.shape, o.dtype) for o in outs[:5]) + (pltpu.HBM((1,), F32),),
        in_specs=[vmem] * 6,
        out_specs=(hbm,) * 6,
        scratch_shapes=[pltpu.SMEM((1,), F32), dma((6,))],
        compiler_params=pltpu.CompilerParams(vmem_limit_bytes=8 * 1024 * 1024),
        name="put_out",
    )(*outs)
    return tuple(final[:5]) + (final[5].reshape(()),)


def solution(mesh):
    in_specs = (
        P("gx", "gy", None),
        P(None, "gx", "gy", None),
        P("gx", "gy", None),
        P(("gx", "gy")),
        P(None, ("gx", "gy")),
        P(("gx", "gy")),
        P(None, ("gx", "gy")),
        P(("gx", "gy")),
    )
    out_specs = (
        P("gx", "gy", None),
        P(None, "gx", "gy", None),
        P("gx", "gy", None),
        P(None, ("gx", "gy")),
        P(None, ("gx", "gy")),
        P(),
    )
    return jax.shard_map(
        functools.partial(on_device, mesh.shape["gx"], mesh.shape["gy"]),
        mesh=mesh, in_specs=in_specs, out_specs=out_specs, check_vma=False,
    )
```

```python
import functools

import jax
import jax.numpy as jnp
from jax import lax
from jax.experimental import pallas as pl
from jax.experimental.pallas import tpu as pltpu
from jax.sharding import PartitionSpec as P

ADIABATIC_INDEX = 1.4
KICK = 0.25
COURANT = 0.4
SHRINK = 0.5
MESH = pl.DeviceIdType.MESH
CHUNK = 1024
F32 = jnp.float32
BF16 = jnp.bfloat16
F8 = jnp.float8_e4m3fn
LIFT = 2048.0
SEND_AT = 2
HUB_GX, HUB_GY = 1, 0


def dot_nt(a, b):
    return lax.dot_general(a, b, (((1,), (1,)), ((), ())), preferred_element_type=F32)


def two_terms(x):
    high = x.astype(BF16)
    low = (x - high.astype(F32)).astype(BF16)
    return high, low


def one_hot_rows(row, count):
    lanes = row.shape[1]
    base = (
        jnp.broadcast_to(row, (16, lanes))
        - lax.broadcasted_iota(jnp.int32, (16, lanes), 0).astype(F32)
    ).astype(BF16)
    one, zero = jnp.ones((16, lanes), BF16), jnp.zeros((16, lanes), BF16)
    return jnp.concatenate(
        [jnp.where(base == 16.0 * k, one, zero) for k in range(count // 16)], axis=0
    )


def kernel(
    n_gx, n_gy, count_hbm, density_hbm, momentum_hbm, energy_hbm, mass_hbm, vel_hbm, temp_hbm, cell_hbm,
    rho_ref, imp_ref, en_ref, state_ref, moved_ref, step_ref,
    src_ref, pay_ref, col_ref, q_ref, r_ref, g0_ref, g1_ref, h0_ref, h1_ref, a0_ref, a1_ref, c0_ref, c1_ref, e0_ref, e1_ref, f0_ref, f1_ref,
    b0_ref, b1_ref, d0_ref, d1_ref, acc_ref, low_ref, small_ref,
    out_bucket, in_bucket, out_face, in_face, own_ref, max_z, max_p, max_h,
    bucket_send, bucket_recv, face_send, face_recv, mz_send, mz_recv, mp_send, mp_recv, mh_send, mh_recv,
    count_ref, density_ref, momentum_ref, energy_ref, mass_ref, vel_ref, temp_ref, cell_ref, load_sem,
):
    sources = (count_hbm, mass_hbm, temp_hbm, vel_hbm, cell_hbm, energy_hbm, density_hbm, momentum_hbm)
    places = (count_ref, mass_ref, temp_ref, vel_ref, cell_ref, energy_ref, density_ref, momentum_ref)
    loads = []
    for k in range(8):
        load = pltpu.make_async_copy(sources[k], places[k], load_sem.at[k])
        load.start()
        loads.append(load)
    gx, gy = lax.axis_index("gx"), lax.axis_index("gy")
    cx, cy, nz = density_ref.shape
    rows = mass_ref.shape[1]
    cap = rows // 16
    per = cap // 128

    half = n_gy // 2
    upper_half, plane = gy // half, lax.rem(gy, half)
    in_column, n_column = upper_half * n_gx + gx, 2 * n_gx

    def column_peer(k):
        place = lax.rem(in_column + k, n_column)
        return {"gx": lax.rem(place, n_gx), "gy": place // n_gx * half + plane}

    def plane_peer(k):
        return {"gy": upper_half * half + lax.rem(plane + k, half)}

    targets = (
        {"gx": lax.rem(gx + n_gx - 1, n_gx)},
        {"gx": lax.rem(gx + 1, n_gx)},
        {"gy": lax.rem(gy + n_gy - 1, n_gy)},
        {"gy": lax.rem(gy + 1, n_gy)},
    )
    landing = (1, 0, 3, 2)

    barrier = pltpu.get_barrier_semaphore()
    greeted = [column_peer(k) for k in range(1, n_column)] + [plane_peer(k) for k in range(1, half)] + list(targets[2:])
    for peer in greeted:
        pl.semaphore_signal(barrier, inc=1, device_id=peer, device_id_type=MESH)

    devices = n_gx * n_gy
    is_hub = (gx == HUB_GX) & (gy == HUB_GY)
    not_hub = jnp.logical_not(is_hub)
    hub = HUB_GY * n_gx + HUB_GX
    hub_slot = lax.rem(gy * n_gx + gx + devices - hub - 1, devices)

    @pl.when(is_hub)
    def _():
        def greet(k, carry):
            other = lax.rem(k + hub + 1, devices)
            peer = {"gx": lax.rem(other, n_gx), "gy": other // n_gx}
            pl.semaphore_signal(barrier, inc=1, device_id=peer, device_id_type=MESH)
            return carry

        lax.fori_loop(0, devices - 1, greet, 0)

    for zeroed in (small_ref, acc_ref, low_ref):
        zeroed[...] = jnp.zeros_like(zeroed)
    for load in loads[:5]:
        load.wait()
    mass, temp = mass_ref[...], temp_ref[...]
    live = lax.broadcasted_iota(jnp.int32, (1, rows), 1) < jnp.broadcast_to(count_ref[...], (1, rows))
    evap = jnp.where(live, mass * jax.nn.sigmoid(2.0 * (temp - 2.0)), 0.0)
    vx, vy, vz = vel_ref[0:1, :], vel_ref[1:2, :], vel_ref[2:3, :]
    src_ref[0:1, :] = evap
    src_ref[1:2, :] = evap * vx
    src_ref[2:3, :] = evap * vy
    src_ref[3:4, :] = evap * vz
    src_ref[4:5, :] = evap * (temp + 0.5 * (vx * vx + vy * vy + vz * vz))
    pay_ref[0:1, :] = mass - SHRINK * evap
    pay_ref[1:4, :] = vel_ref[...]
    pay_ref[4:5, :] = temp
    pay_ref[5:8, :] = cell_ref[...].astype(F32)
    lx = cell_ref[0:1, :] - gx * cx
    ly = cell_ref[1:2, :] - gy * cy
    heading = jnp.where(
        lx < 0, 0, jnp.where(lx >= cx, 1, jnp.where(ly < 0, 2, jnp.where(ly >= cy, 3, 4)))
    )
    heading = jnp.where(live, heading, 5)
    stays = heading == 4
    col_ref[...] = jnp.where(stays, lx * cy + ly, -1000).astype(F32)
    state_ref[:, :rows] = jnp.where(stays, pay_ref[0:5, :], 0.0)
    moved_ref[:, :rows] = jnp.where(stays, cell_ref[...], 0)

    blocks = rows // 128
    marks = jnp.where(
        jnp.broadcast_to(heading, (8, rows)) == lax.broadcasted_iota(jnp.int32, (8, rows), 0), 1.0, 0.0
    )
    stacked = jnp.concatenate([marks[:, k * 128 : (k + 1) * 128] for k in range(blocks)], axis=0)
    i0 = lax.broadcasted_iota(jnp.int32, (128, 256), 0)
    i1 = lax.broadcasted_iota(jnp.int32, (128, 256), 1)
    upper = jnp.where((i0 < i1) | (i1 >= 128), 1.0, 0.0).astype(BF16)
    sums = jnp.dot(stacked.astype(BF16), upper, preferred_element_type=F32)
    carry = jnp.zeros((8, 128), F32)
    ranks = []
    for k in range(blocks):
        part = sums[k * 8 : (k + 1) * 8]
        mark = stacked[k * 8 : (k + 1) * 8]
        ranks.append(jnp.sum((part[:, :128] + carry) * mark, axis=0, keepdims=True))
        carry = carry + part[:, 128:]
    rank = jnp.concatenate(ranks, axis=1).astype(jnp.int32)
    q_ref[...] = jnp.where(heading < 4, heading * per + (rank >> 7), -1).astype(F32)
    r_ref[...] = (rank & 127).astype(F32)

    inside = (gx > 0, gx < n_gx - 1, gy > 0, gy < n_gy - 1)

    def exchange(src, dst, send, recv):
        copies = []
        for h in range(4):
            copy = pltpu.make_async_remote_copy(
                src_ref=src.at[h], dst_ref=dst.at[landing[h]], send_sem=send.at[h],
                recv_sem=recv.at[landing[h]], device_id=targets[h], device_id_type=MESH,
            )
            copies.append(copy)
        return copies

    def send(copies, which):
        for h in which:
            pl.when(inside[h])(copies[h].start)

    def wait_received(copies, which):
        for h in which:
            pl.when(inside[landing[h]])(copies[h].wait_recv)

    for b in range(4):
        @pl.when(jnp.logical_not(inside[b]))
        def _():
            in_bucket[b] = jnp.zeros(in_bucket.shape[1:], F32)

    cells = cx * cy
    chunks = rows // CHUNK
    groups = 4 * per

    def spread(lanes, values, a_ref, c_ref):
        base = (
            jnp.broadcast_to(col_ref[:, lanes], (16, CHUNK))
            - lax.broadcasted_iota(jnp.int32, (16, CHUNK), 0).astype(F32)
        ).astype(BF16)
        zero = jnp.zeros((16, CHUNK), BF16)
        hits = [base == 16.0 * k for k in range(cells // 16)]
        for n, v in enumerate(values):
            value = jnp.broadcast_to(src_ref[v : v + 1, lanes], (16, CHUNK))
            high = value.astype(BF16)
            low = ((value - high.astype(F32)) * LIFT).astype(BF16)
            for k in range(cells // 16):
                at = n * cells + k * 16
                a_ref[at : at + 16, :] = jnp.where(hits[k], high, zero)
            for k in range(0, cells // 16, 2):
                at = n * cells + k * 16
                pair = jnp.concatenate([jnp.where(hits[k], low, zero), jnp.where(hits[k + 1], low, zero)], axis=0)
                c_ref[at : at + 32, :] = pair.astype(F8)

    def chunk_of(c):
        if isinstance(c, int):
            return slice(c * CHUNK, (c + 1) * CHUNK)
        return pl.ds(pl.multiple_of(c * CHUNK, CHUNK), CHUNK)

    def build_pack(c, g_ref, h_ref):
        lanes = chunk_of(c)
        high, low = two_terms(pay_ref[:, lanes])
        both = jnp.concatenate([high.astype(F32), low.astype(F32)], axis=0).astype(BF16)
        q = jnp.broadcast_to(q_ref[:, lanes], (16, CHUNK)).astype(BF16)
        zero = jnp.zeros((16, CHUNK), BF16)
        for k in range(groups):
            g_ref[k * 16 : (k + 1) * 16, :] = jnp.where(q == float(k), both, zero)
        h_ref[...] = one_hot_rows(r_ref[:, lanes], 128)

    build_pack(0, g0_ref, h0_ref)

    def two_packs(i, carry):
        small_ref[...] += dot_nt(g0_ref[...], h0_ref[...])
        build_pack(2 * i + 1, g1_ref, h1_ref)
        small_ref[...] += dot_nt(g1_ref[...], h1_ref[...])
        build_pack(jnp.minimum(2 * i + 2, chunks - 1), g0_ref, h0_ref)
        return carry

    lax.fori_loop(0, chunks // 2, two_packs, 0)
    for h in range(4):
        for j in range(per):
            k = (h * per + j) * 16
            out_bucket[h, :, j * 128 : (j + 1) * 128] = small_ref[k : k + 8, :] + small_ref[k + 8 : k + 16, :]

    moves = exchange(out_bucket, in_bucket, bucket_send, bucket_recv)
    faces = exchange(out_face, in_face, face_send, face_recv)

    e_rows = slice(4 * cells, 5 * cells)

    def build_energy(c, i, a_ref, c_ref, b_ref, d_ref):
        lanes, place = chunk_of(c), chunk_of(i)
        spread(lanes, (4,), a_ref, c_ref)
        depth = one_hot_rows(cell_ref[2:3, lanes].astype(F32), nz)
        b_ref[:, place] = depth
        d_ref[:, place] = depth.astype(F8)

    build_energy(0, 0, e0_ref, f0_ref, b0_ref, d0_ref)

    def send_moves():
        pl.when(is_hub)(lambda: pl.semaphore_wait(barrier, len(greeted)))
        pl.when(not_hub)(lambda: pl.semaphore_wait(barrier, len(greeted) + 1))
        send(moves, (2, 3, 0, 1))

    def two_energy(i, carry):
        pl.when(i == SEND_AT)(send_moves)
        place = chunk_of(i)
        acc_ref[e_rows, :] += dot_nt(e0_ref[...], b0_ref[:, place])
        low_ref[e_rows, :] += dot_nt(f0_ref[...], d0_ref[:, place])
        build_energy(2 * i + 1, i, e1_ref, f1_ref, b1_ref, d1_ref)
        acc_ref[e_rows, :] += dot_nt(e1_ref[...], b1_ref[:, place])
        low_ref[e_rows, :] += dot_nt(f1_ref[...], d1_ref[:, place])
        later = jnp.minimum(i + 1, chunks // 2 - 1)
        build_energy(2 * later, later, e0_ref, f0_ref, b0_ref, d0_ref)
        return carry

    lax.fori_loop(0, chunks // 2, two_energy, 0)

    def sums_of(got, b, with_all):
        warm = got[4:5]
        share = jax.nn.sigmoid(2.0 * (warm - 2.0))
        boiled = got[0:1] * share / (1.0 - SHRINK * share)
        speed = got[1:4]
        budget = 0.5 * jnp.sum(speed * speed, axis=0, keepdims=True)
        values = [boiled * (warm + budget)]
        if with_all:
            values = [boiled] + [boiled * got[k : k + 1] for k in (1, 2, 3)] + values
        if b < 2:
            along = got[6:7] - (gy * cy).astype(F32)
        else:
            along = got[5:6] - (gx * cx).astype(F32)
        hit = (
            jnp.broadcast_to(along, (16, cap))
            == lax.broadcasted_iota(jnp.int32, (16, cap), 0).astype(F32)
        )
        parts = []
        for value in values:
            wide = jnp.where(hit, jnp.broadcast_to(value, (16, cap)), 0.0)
            parts.append(two_terms(wide))
        left = jnp.concatenate([p[0] for p in parts] + [p[1] for p in parts], axis=0)
        sums = dot_nt(left, one_hot_rows(got[7:8], nz))
        n = len(values) * 16
        return sums[0:n] + sums[n : 2 * n]

    def receive(b):
        got = in_bucket[b]
        state_ref[:, rows + b * cap : rows + (b + 1) * cap] = got[0:5]
        moved_ref[:, rows + b * cap : rows + (b + 1) * cap] = got[5:8].astype(jnp.int32)
        sums = sums_of(got, b, True)
        for v in range(5):
            part = sums[v * 16 : (v + 1) * 16]
            if b < 2:
                at = v * cells + (0 if b == 0 else (cx - 1) * cy)
                acc_ref[at : at + cy, :] += part
            else:
                edge = 0 if b == 2 else cy - 1
                for x in range(cx):
                    at = v * cells + x * cy + edge
                    acc_ref[at : at + 1, :] += part[x : x + 1]

    def deposit(v):
        at = slice(v * cells, (v + 1) * cells)
        return (acc_ref[at, :] + low_ref[at, :] * (1.0 / LIFT)).reshape(cx, cy, nz)

    def receive_x():
        wait_received(moves, (0, 1))
        receive(0)
        receive(1)
        for load in loads[5:]:
            load.wait()
        energy = energy_ref[...] + deposit(4)
        for x in range(cx):
            out_face[2, x : x + 1, :] = (ADIABATIC_INDEX - 1.0) * energy[x, 0:1, :]
            out_face[3, x : x + 1, :] = (ADIABATIC_INDEX - 1.0) * energy[x, cy - 1 : cy, :]
        send(faces, (2, 3))

    def receive_y():
        wait_received(moves, (2, 3))
        receive(2)
        receive(3)
        for h in (2, 3):
            own_ref[h - 2] = (ADIABATIC_INDEX - 1.0) * sums_of(out_bucket[h], h, False)
        energy = energy_ref[...] + deposit(4)
        en_ref[...] = energy
        out_face[0] = (ADIABATIC_INDEX - 1.0) * energy[0]
        out_face[1] = (ADIABATIC_INDEX - 1.0) * energy[cx - 1]
        send(faces, (0, 1))

    others = slice(0, 4 * cells)
    spread(chunk_of(0), (0, 1, 2, 3), a0_ref, c0_ref)

    def two_others(i, carry):
        pl.when(i == 1)(receive_x)
        pl.when(i == 2)(receive_y)
        place = chunk_of(i)
        acc_ref[others, :] += dot_nt(a0_ref[...], b0_ref[:, place])
        low_ref[others, :] += dot_nt(c0_ref[...], d0_ref[:, place])
        spread(chunk_of(2 * i + 1), (0, 1, 2, 3), a1_ref, c1_ref)
        acc_ref[others, :] += dot_nt(a1_ref[...], b1_ref[:, place])
        low_ref[others, :] += dot_nt(c1_ref[...], d1_ref[:, place])
        spread(chunk_of(jnp.minimum(2 * i + 2, chunks - 1)), (0, 1, 2, 3), a0_ref, c0_ref)
        return carry

    lax.fori_loop(0, chunks // 2, two_others, 0)

    pressure = (ADIABATIC_INDEX - 1.0) * en_ref[...]
    density = density_ref[...] + deposit(0)
    rho_ref[...] = density
    lane = lax.broadcasted_iota(jnp.int32, (cx, cy, nz), 2)
    after = jnp.where(lane == nz - 1, 0.0, pltpu.roll(pressure, nz - 1, 2))
    before = jnp.where(lane == 0, 0.0, pltpu.roll(pressure, 1, 2))
    impulse_z = momentum_ref[2] + deposit(3) - KICK * (0.5 * (after - before))
    imp_ref[2] = impulse_z
    sound = jnp.sqrt(ADIABATIC_INDEX * pressure / density)
    wait_received(faces, range(4))
    low_x = jnp.where(gx > 0, in_face[0], 0.0)
    high_x = jnp.where(gx < n_gx - 1, in_face[1], 0.0)
    low_y = jnp.where(gy > 0, in_face[2] + own_ref[0], 0.0)
    high_y = jnp.where(gy < n_gy - 1, in_face[3] + own_ref[1], 0.0)
    after = jnp.concatenate([pressure[1:], high_x[None]], axis=0)
    before = jnp.concatenate([low_x[None], pressure[:-1]], axis=0)
    impulse_x = momentum_ref[0] + deposit(1) - KICK * (0.5 * (after - before))
    imp_ref[0] = impulse_x
    line = lax.broadcasted_iota(jnp.int32, (cx, cy, nz), 1)
    after = jnp.where(line == cy - 1, high_y[:, None, :], pltpu.roll(pressure, cy - 1, 1))
    before = jnp.where(line == 0, low_y[:, None, :], pltpu.roll(pressure, 1, 1))
    impulse_y = momentum_ref[1] + deposit(2) - KICK * (0.5 * (after - before))
    imp_ref[1] = impulse_y
    fastest = jnp.maximum(jnp.maximum(jnp.abs(impulse_x), jnp.abs(impulse_y)), jnp.abs(impulse_z))
    wave = fastest / density + sound

    def share_max(me, n, peer, slots, send, recv):
        copies = []
        for k in range(1, n):
            copies.append(pltpu.make_async_remote_copy(
                src_ref=slots.at[me], dst_ref=slots.at[me], send_sem=send.at[k],
                recv_sem=recv.at[k], device_id=peer(k), device_id_type=MESH,
            ))
        return copies

    top = jnp.max(jnp.max(wave, axis=0), axis=0, keepdims=True)
    max_p[plane] = jnp.maximum(top[:, 0:128], top[:, 128:256])
    to_hub = pltpu.make_async_remote_copy(
        src_ref=max_p.at[plane], dst_ref=max_h.at[hub_slot], send_sem=mh_send.at[0],
        recv_sem=mh_recv.at[0], device_id={"gx": HUB_GX, "gy": HUB_GY}, device_id_type=MESH,
    )
    pl.when(not_hub)(to_hub.start)
    sent_p = share_max(plane, half, plane_peer, max_p, mp_send, mp_recv)
    for copy in sent_p:
        copy.start()
    for copy in sent_p:
        copy.wait_recv()
    max_z[in_column] = jnp.max(max_p[...], axis=0)
    sent_z = share_max(in_column, n_column, column_peer, max_z, mz_send, mz_recv)
    for k in range(1, n_column):
        peer = column_peer(k)
        to_other = jnp.logical_not((peer["gx"] == HUB_GX) & (peer["gy"] == HUB_GY))
        pl.when(to_other)(sent_z[k - 1].start)

    @pl.when(not_hub)
    def _():
        for copy in sent_z:
            copy.wait_recv()
        step_ref[...] = COURANT / jnp.broadcast_to(jnp.max(max_z[...]), (1, 128))

    @pl.when(is_hub)
    def _():
        arrived = max_h.at[pl.ds(0, devices - 1)]
        pltpu.make_async_remote_copy(
            src_ref=arrived, dst_ref=arrived, send_sem=mh_send.at[0], recv_sem=mh_recv.at[0],
            device_id={"gx": HUB_GX, "gy": HUB_GY}, device_id_type=MESH,
        ).wait_recv()
        best = jnp.maximum(jnp.max(arrived[...], axis=0), max_p[plane])
        step_ref[...] = COURANT / jnp.broadcast_to(jnp.max(best), (1, 128))

    pl.when(not_hub)(to_hub.wait_send)
    for k in range(1, n_column):
        peer = column_peer(k)
        to_other = jnp.logical_not((peer["gx"] == HUB_GX) & (peer["gy"] == HUB_GY))
        pl.when(to_other)(sent_z[k - 1].wait_send)
    for copies in (moves, faces):
        for h in range(4):
            pl.when(inside[h])(copies[h].wait_send)
    for copy in sent_p:
        copy.wait_send()


def put_out(*refs):
    count = (len(refs) - 2) // 2
    step_ref, sem = refs[-2:]
    step_ref[0] = refs[count - 1][0, 0]
    copies = []
    for k in range(count):
        source = refs[k] if k < count - 1 else step_ref
        copy = pltpu.make_async_copy(source, refs[count + k], sem.at[k])
        copy.start()
        copies.append(copy)
    for copy in copies:
        copy.wait()


def on_device(n_gx, n_gy, density, momentum, energy, mass, velocity, temp, cell, count):
    rows = mass.shape[0]
    cap = rows // 16
    slots = rows + 4 * cap
    cx, cy, nz = density.shape
    vmem = pl.BlockSpec(memory_space=pltpu.VMEM)
    hbm = pl.BlockSpec(memory_space=pltpu.HBM)
    cells = cx * cy
    half = n_gy // 2
    dma = pltpu.SemaphoreType.DMA
    outs = pl.pallas_call(
        functools.partial(kernel, n_gx, n_gy),
        out_shape=(
            pltpu.VMEM(density.shape, F32),
            pltpu.VMEM(momentum.shape, F32),
            pltpu.VMEM(energy.shape, F32),
            pltpu.VMEM((5, slots), F32),
            pltpu.VMEM((3, slots), jnp.int32),
            pltpu.VMEM((1, 128), F32),
        ),
        in_specs=[hbm] * 8,
        out_specs=(vmem,) * 6,
        scratch_shapes=[
            pltpu.VMEM((8, rows), F32),
            pltpu.VMEM((8, rows), F32),
            pltpu.VMEM((1, rows), F32),
            pltpu.VMEM((1, rows), F32),
            pltpu.VMEM((1, rows), F32),
            pltpu.VMEM((4 * (cap // 128) * 16, CHUNK), BF16),
            pltpu.VMEM((4 * (cap // 128) * 16, CHUNK), BF16),
            pltpu.VMEM((128, CHUNK), BF16),
            pltpu.VMEM((128, CHUNK), BF16),
            pltpu.VMEM((4 * cells, CHUNK), BF16),
            pltpu.VMEM((4 * cells, CHUNK), BF16),
            pltpu.VMEM((4 * cells, CHUNK), F8),
            pltpu.VMEM((4 * cells, CHUNK), F8),
            pltpu.VMEM((cells, CHUNK), BF16),
            pltpu.VMEM((cells, CHUNK), BF16),
            pltpu.VMEM((cells, CHUNK), F8),
            pltpu.VMEM((cells, CHUNK), F8),
            pltpu.VMEM((nz, rows // 2), BF16),
            pltpu.VMEM((nz, rows // 2), BF16),
            pltpu.VMEM((nz, rows // 2), F8),
            pltpu.VMEM((nz, rows // 2), F8),
            pltpu.VMEM((5 * cells, nz), F32),
            pltpu.VMEM((5 * cells, nz), F32),
            pltpu.VMEM((4 * (cap // 128) * 16, 128), F32),
            pltpu.VMEM((4, 8, cap), F32),
            pltpu.VMEM((4, 8, cap), F32),
            pltpu.VMEM((4, cx, nz), F32),
            pltpu.VMEM((4, cx, nz), F32),
            pltpu.VMEM((2, cx, nz), F32),
            pltpu.VMEM((2 * n_gx, 1, 128), F32),
            pltpu.VMEM((half, 1, 128), F32),
            pltpu.VMEM((n_gx * n_gy, 1, 128), F32),
            dma((4,)),
            dma((4,)),
            dma((4,)),
            dma((4,)),
            dma((2 * n_gx,)),
            dma((2 * n_gx,)),
            dma((half,)),
            dma((half,)),
            dma((1,)),
            dma((1,)),
            pltpu.VMEM((1, 1), jnp.int32),
            pltpu.VMEM(density.shape, F32),
            pltpu.VMEM(momentum.shape, F32),
            pltpu.VMEM(energy.shape, F32),
            pltpu.VMEM((1, rows), F32),
            pltpu.VMEM(velocity.shape, F32),
            pltpu.VMEM((1, rows), F32),
            pltpu.VMEM(cell.shape, jnp.int32),
            dma((8,)),
        ],
        compiler_params=pltpu.CompilerParams(
            collective_id=0, has_side_effects=True, vmem_limit_bytes=64200000
        ),
        name="spray",
    )(count.reshape(1, 1), density, momentum, energy, mass.reshape(1, rows), velocity, temp.reshape(1, rows), cell)
    final = pl.pallas_call(
        put_out,
        out_shape=tuple(pltpu.HBM(o.shape, o.dtype) for o in outs[:5]) + (pltpu.HBM((1,), F32),),
        in_specs=[vmem] * 6,
        out_specs=(hbm,) * 6,
        scratch_shapes=[pltpu.SMEM((1,), F32), dma((6,))],
        compiler_params=pltpu.CompilerParams(vmem_limit_bytes=8 * 1024 * 1024),
        name="put_out",
    )(*outs)
    return tuple(final[:5]) + (final[5].reshape(()),)


def solution(mesh):
    in_specs = (
        P("gx", "gy", None),
        P(None, "gx", "gy", None),
        P("gx", "gy", None),
        P(("gx", "gy")),
        P(None, ("gx", "gy")),
        P(("gx", "gy")),
        P(None, ("gx", "gy")),
        P(("gx", "gy")),
    )
    out_specs = (
        P("gx", "gy", None),
        P(None, "gx", "gy", None),
        P("gx", "gy", None),
        P(None, ("gx", "gy")),
        P(None, ("gx", "gy")),
        P(),
    )
    return jax.shard_map(
        functools.partial(on_device, mesh.shape["gx"], mesh.shape["gy"]),
        mesh=mesh, in_specs=in_specs, out_specs=out_specs, check_vma=False,
    )
```

```python
import functools

import jax
import jax.numpy as jnp
from jax import lax
from jax.experimental import pallas as pl
from jax.experimental.pallas import tpu as pltpu
from jax.sharding import PartitionSpec as P

ADIABATIC_INDEX = 1.4
KICK = 0.25
COURANT = 0.4
SHRINK = 0.5
MESH = pl.DeviceIdType.MESH
CHUNK = 1024
F32 = jnp.float32
BF16 = jnp.bfloat16
F8 = jnp.float8_e4m3fn
LIFT = 2048.0
HUBS = ((1, 0), (0, 1), (1, 1), (0, 4), (1, 4), (2, 0), (3, 0))


def dot_nt(a, b):
    return lax.dot_general(a, b, (((1,), (1,)), ((), ())), preferred_element_type=F32)


def two_terms(x):
    high = x.astype(BF16)
    low = (x - high.astype(F32)).astype(BF16)
    return high, low


def one_hot_rows(row, count):
    lanes = row.shape[1]
    base = (
        jnp.broadcast_to(row, (16, lanes))
        - lax.broadcasted_iota(jnp.int32, (16, lanes), 0).astype(F32)
    ).astype(BF16)
    one, zero = jnp.ones((16, lanes), BF16), jnp.zeros((16, lanes), BF16)
    return jnp.concatenate(
        [jnp.where(base == 16.0 * k, one, zero) for k in range(count // 16)], axis=0
    )


def kernel(
    n_gx, n_gy, count_hbm, density_hbm, momentum_hbm, energy_hbm, mass_hbm, vel_hbm, temp_hbm, cell_hbm,
    rho_ref, imp_ref, en_ref, state_ref, moved_ref, step_ref,
    src_ref, pay_ref, col_ref, q_ref, r_ref, g0_ref, g1_ref, h0_ref, h1_ref, a0_ref, a1_ref, c0_ref, c1_ref, e0_ref, e1_ref, f0_ref, f1_ref,
    b0_ref, b1_ref, d0_ref, d1_ref, acc_ref, low_ref, small_ref,
    out_bucket, in_bucket, out_face, in_face, own_ref, max_z, max_p, max_h,
    bucket_send, bucket_recv, face_send, face_recv, mz_send, mz_recv, mp_send, mp_recv, mh_send, mh_recv,
    count_ref, density_ref, momentum_ref, energy_ref, mass_ref, vel_ref, temp_ref, cell_ref, load_sem,
):
    sources = (count_hbm, mass_hbm, temp_hbm, vel_hbm, cell_hbm, energy_hbm, density_hbm, momentum_hbm)
    places = (count_ref, mass_ref, temp_ref, vel_ref, cell_ref, energy_ref, density_ref, momentum_ref)
    loads = []
    for k in range(8):
        load = pltpu.make_async_copy(sources[k], places[k], load_sem.at[k])
        load.start()
        loads.append(load)
    gx, gy = lax.axis_index("gx"), lax.axis_index("gy")
    cx, cy, nz = density_ref.shape
    rows = mass_ref.shape[1]
    cap = rows // 16
    per = cap // 128

    half = n_gy // 2
    upper_half, plane = gy // half, lax.rem(gy, half)
    in_column, n_column = upper_half * n_gx + gx, 2 * n_gx

    def column_peer(k):
        place = lax.rem(in_column + k, n_column)
        return {"gx": lax.rem(place, n_gx), "gy": place // n_gx * half + plane}

    def plane_peer(k):
        return {"gy": upper_half * half + lax.rem(plane + k, half)}

    targets = (
        {"gx": lax.rem(gx + n_gx - 1, n_gx)},
        {"gx": lax.rem(gx + 1, n_gx)},
        {"gy": lax.rem(gy + n_gy - 1, n_gy)},
        {"gy": lax.rem(gy + 1, n_gy)},
    )
    landing = (1, 0, 3, 2)

    barrier = pltpu.get_barrier_semaphore()
    greeted = [column_peer(k) for k in range(1, n_column)] + [plane_peer(k) for k in range(1, half)] + list(targets[2:])
    for peer in greeted:
        pl.semaphore_signal(barrier, inc=1, device_id=peer, device_id_type=MESH)

    devices = n_gx * n_gy

    def is_at(place, spots):
        found = jnp.bool_(False)
        for spot in spots:
            found = found | ((place[0] == spot[0]) & (place[1] == spot[1]))
        return found

    is_hub = is_at((gx, gy), HUBS)
    not_hub = jnp.logical_not(is_hub)
    me = gy * n_gx + gx

    @pl.when(is_hub)
    def _():
        def greet(j, carry):
            for k in range(15):
                other = lax.rem(j * 15 + k + me + 1, devices)
                peer = {"gx": lax.rem(other, n_gx), "gy": other // n_gx}
                pl.semaphore_signal(barrier, inc=1, device_id=peer, device_id_type=MESH)
            return carry

        lax.fori_loop(0, (devices - 1) // 15, greet, 0)

    for zeroed in (small_ref, acc_ref, low_ref):
        zeroed[...] = jnp.zeros_like(zeroed)
    for load in loads[:5]:
        load.wait()
    mass, temp = mass_ref[...], temp_ref[...]
    live = lax.broadcasted_iota(jnp.int32, (1, rows), 1) < jnp.broadcast_to(count_ref[...], (1, rows))
    evap = jnp.where(live, mass * jax.nn.sigmoid(2.0 * (temp - 2.0)), 0.0)
    vx, vy, vz = vel_ref[0:1, :], vel_ref[1:2, :], vel_ref[2:3, :]
    src_ref[0:1, :] = evap
    src_ref[1:2, :] = evap * vx
    src_ref[2:3, :] = evap * vy
    src_ref[3:4, :] = evap * vz
    src_ref[4:5, :] = evap * (temp + 0.5 * (vx * vx + vy * vy + vz * vz))
    pay_ref[0:1, :] = mass - SHRINK * evap
    pay_ref[1:4, :] = vel_ref[...]
    pay_ref[4:5, :] = temp
    pay_ref[5:8, :] = cell_ref[...].astype(F32)
    lx = cell_ref[0:1, :] - gx * cx
    ly = cell_ref[1:2, :] - gy * cy
    heading = jnp.where(
        lx < 0, 0, jnp.where(lx >= cx, 1, jnp.where(ly < 0, 2, jnp.where(ly >= cy, 3, 4)))
    )
    heading = jnp.where(live, heading, 5)
    stays = heading == 4
    col_ref[...] = jnp.where(stays, lx * cy + ly, -1000).astype(F32)
    state_ref[:, :rows] = jnp.where(stays, pay_ref[0:5, :], 0.0)
    moved_ref[:, :rows] = jnp.where(stays, cell_ref[...], 0)

    blocks = rows // 128
    marks = jnp.where(
        jnp.broadcast_to(heading, (8, rows)) == lax.broadcasted_iota(jnp.int32, (8, rows), 0), 1.0, 0.0
    )
    stacked = jnp.concatenate([marks[:, k * 128 : (k + 1) * 128] for k in range(blocks)], axis=0)
    i0 = lax.broadcasted_iota(jnp.int32, (128, 256), 0)
    i1 = lax.broadcasted_iota(jnp.int32, (128, 256), 1)
    upper = jnp.where((i0 < i1) | (i1 >= 128), 1.0, 0.0).astype(BF16)
    sums = jnp.dot(stacked.astype(BF16), upper, preferred_element_type=F32)
    carry = jnp.zeros((8, 128), F32)
    ranks = []
    for k in range(blocks):
        part = sums[k * 8 : (k + 1) * 8]
        mark = stacked[k * 8 : (k + 1) * 8]
        ranks.append(jnp.sum((part[:, :128] + carry) * mark, axis=0, keepdims=True))
        carry = carry + part[:, 128:]
    rank = jnp.concatenate(ranks, axis=1).astype(jnp.int32)
    q_ref[...] = jnp.where(heading < 4, heading * per + (rank >> 7), -1).astype(F32)
    r_ref[...] = (rank & 127).astype(F32)

    inside = (gx > 0, gx < n_gx - 1, gy > 0, gy < n_gy - 1)

    def exchange(src, dst, send, recv):
        copies = []
        for h in range(4):
            copy = pltpu.make_async_remote_copy(
                src_ref=src.at[h], dst_ref=dst.at[landing[h]], send_sem=send.at[h],
                recv_sem=recv.at[landing[h]], device_id=targets[h], device_id_type=MESH,
            )
            copies.append(copy)
        return copies

    def send(copies, which):
        for h in which:
            pl.when(inside[h])(copies[h].start)

    def wait_received(copies, which):
        for h in which:
            pl.when(inside[landing[h]])(copies[h].wait_recv)

    for b in range(4):
        @pl.when(jnp.logical_not(inside[b]))
        def _():
            in_bucket[b] = jnp.zeros(in_bucket.shape[1:], F32)

    cells = cx * cy
    chunks = rows // CHUNK
    groups = 4 * per

    def spread(lanes, values, a_ref, c_ref):
        base = (
            jnp.broadcast_to(col_ref[:, lanes], (16, CHUNK))
            - lax.broadcasted_iota(jnp.int32, (16, CHUNK), 0).astype(F32)
        ).astype(BF16)
        zero = jnp.zeros((16, CHUNK), BF16)
        hits = [base == 16.0 * k for k in range(cells // 16)]
        for n, v in enumerate(values):
            value = jnp.broadcast_to(src_ref[v : v + 1, lanes], (16, CHUNK))
            high = value.astype(BF16)
            low = ((value - high.astype(F32)) * LIFT).astype(BF16)
            for k in range(cells // 16):
                at = n * cells + k * 16
                a_ref[at : at + 16, :] = jnp.where(hits[k], high, zero)
            for k in range(0, cells // 16, 2):
                at = n * cells + k * 16
                pair = jnp.concatenate([jnp.where(hits[k], low, zero), jnp.where(hits[k + 1], low, zero)], axis=0)
                c_ref[at : at + 32, :] = pair.astype(F8)

    def chunk_of(c):
        if isinstance(c, int):
            return slice(c * CHUNK, (c + 1) * CHUNK)
        return pl.ds(pl.multiple_of(c * CHUNK, CHUNK), CHUNK)

    def build_pack(c, g_ref, h_ref):
        lanes = chunk_of(c)
        high, low = two_terms(pay_ref[:, lanes])
        both = jnp.concatenate([high.astype(F32), low.astype(F32)], axis=0).astype(BF16)
        q = jnp.broadcast_to(q_ref[:, lanes], (16, CHUNK)).astype(BF16)
        zero = jnp.zeros((16, CHUNK), BF16)
        for k in range(groups):
            g_ref[k * 16 : (k + 1) * 16, :] = jnp.where(q == float(k), both, zero)
        h_ref[...] = one_hot_rows(r_ref[:, lanes], 128)

    build_pack(0, g0_ref, h0_ref)

    moves = exchange(out_bucket, in_bucket, bucket_send, bucket_recv)
    faces = exchange(out_face, in_face, face_send, face_recv)

    e_rows = slice(4 * cells, 5 * cells)

    def build_energy(c, i, a_ref, c_ref, b_ref, d_ref):
        lanes, place = chunk_of(c), chunk_of(i)
        spread(lanes, (4,), a_ref, c_ref)
        depth = one_hot_rows(cell_ref[2:3, lanes].astype(F32), nz)
        b_ref[:, place] = depth
        d_ref[:, place] = depth.astype(F8)

    build_energy(0, 0, e0_ref, f0_ref, b0_ref, d0_ref)

    def send_moves():
        pl.when(is_hub)(lambda: pl.semaphore_wait(barrier, len(greeted) + len(HUBS) - 1))
        pl.when(not_hub)(lambda: pl.semaphore_wait(barrier, len(greeted) + len(HUBS)))
        send(moves, (2, 3, 0, 1))

    def two_energy(i, carry):
        place = chunk_of(i)
        acc_ref[e_rows, :] += dot_nt(e0_ref[...], b0_ref[:, place])
        low_ref[e_rows, :] += dot_nt(f0_ref[...], d0_ref[:, place])
        small_ref[...] += dot_nt(g0_ref[...], h0_ref[...])
        build_energy(2 * i + 1, i, e1_ref, f1_ref, b1_ref, d1_ref)
        build_pack(2 * i + 1, g1_ref, h1_ref)
        acc_ref[e_rows, :] += dot_nt(e1_ref[...], b1_ref[:, place])
        low_ref[e_rows, :] += dot_nt(f1_ref[...], d1_ref[:, place])
        small_ref[...] += dot_nt(g1_ref[...], h1_ref[...])
        later = jnp.minimum(i + 1, chunks // 2 - 1)
        build_energy(2 * later, later, e0_ref, f0_ref, b0_ref, d0_ref)
        build_pack(2 * later, g0_ref, h0_ref)
        return carry

    lax.fori_loop(0, chunks // 2, two_energy, 0)
    for h in range(4):
        for j in range(per):
            k = (h * per + j) * 16
            out_bucket[h, :, j * 128 : (j + 1) * 128] = small_ref[k : k + 8, :] + small_ref[k + 8 : k + 16, :]
    send_moves()

    def sums_of(got, b, with_all):
        warm = got[4:5]
        share = jax.nn.sigmoid(2.0 * (warm - 2.0))
        boiled = got[0:1] * share / (1.0 - SHRINK * share)
        speed = got[1:4]
        budget = 0.5 * jnp.sum(speed * speed, axis=0, keepdims=True)
        values = [boiled * (warm + budget)]
        if with_all:
            values = [boiled] + [boiled * got[k : k + 1] for k in (1, 2, 3)] + values
        if b < 2:
            along = got[6:7] - (gy * cy).astype(F32)
        else:
            along = got[5:6] - (gx * cx).astype(F32)
        hit = (
            jnp.broadcast_to(along, (16, cap))
            == lax.broadcasted_iota(jnp.int32, (16, cap), 0).astype(F32)
        )
        parts = []
        for value in values:
            wide = jnp.where(hit, jnp.broadcast_to(value, (16, cap)), 0.0)
            parts.append(two_terms(wide))
        left = jnp.concatenate([p[0] for p in parts] + [p[1] for p in parts], axis=0)
        sums = dot_nt(left, one_hot_rows(got[7:8], nz))
        n = len(values) * 16
        return sums[0:n] + sums[n : 2 * n]

    def receive(b):
        got = in_bucket[b]
        state_ref[:, rows + b * cap : rows + (b + 1) * cap] = got[0:5]
        moved_ref[:, rows + b * cap : rows + (b + 1) * cap] = got[5:8].astype(jnp.int32)
        sums = sums_of(got, b, True)
        for v in range(5):
            part = sums[v * 16 : (v + 1) * 16]
            if b < 2:
                at = v * cells + (0 if b == 0 else (cx - 1) * cy)
                acc_ref[at : at + cy, :] += part
            else:
                edge = 0 if b == 2 else cy - 1
                for x in range(cx):
                    at = v * cells + x * cy + edge
                    acc_ref[at : at + 1, :] += part[x : x + 1]

    def deposit(v):
        at = slice(v * cells, (v + 1) * cells)
        return (acc_ref[at, :] + low_ref[at, :] * (1.0 / LIFT)).reshape(cx, cy, nz)

    def receive_x():
        wait_received(moves, (0, 1))
        receive(0)
        receive(1)
        for load in loads[5:]:
            load.wait()
        energy = energy_ref[...] + deposit(4)
        for x in range(cx):
            out_face[2, x : x + 1, :] = (ADIABATIC_INDEX - 1.0) * energy[x, 0:1, :]
            out_face[3, x : x + 1, :] = (ADIABATIC_INDEX - 1.0) * energy[x, cy - 1 : cy, :]
        send(faces, (2, 3))

    def receive_y():
        wait_received(moves, (2, 3))
        receive(2)
        receive(3)
        for h in (2, 3):
            own_ref[h - 2] = (ADIABATIC_INDEX - 1.0) * sums_of(out_bucket[h], h, False)
        energy = energy_ref[...] + deposit(4)
        en_ref[...] = energy
        out_face[0] = (ADIABATIC_INDEX - 1.0) * energy[0]
        out_face[1] = (ADIABATIC_INDEX - 1.0) * energy[cx - 1]
        send(faces, (0, 1))

    others = slice(0, 4 * cells)
    spread(chunk_of(0), (0, 1, 2, 3), a0_ref, c0_ref)

    def two_others(i, carry):
        pl.when(i == 1)(receive_x)
        pl.when(i == 3)(receive_y)
        place = chunk_of(i)
        acc_ref[others, :] += dot_nt(a0_ref[...], b0_ref[:, place])
        low_ref[others, :] += dot_nt(c0_ref[...], d0_ref[:, place])
        spread(chunk_of(2 * i + 1), (0, 1, 2, 3), a1_ref, c1_ref)
        acc_ref[others, :] += dot_nt(a1_ref[...], b1_ref[:, place])
        low_ref[others, :] += dot_nt(c1_ref[...], d1_ref[:, place])
        spread(chunk_of(jnp.minimum(2 * i + 2, chunks - 1)), (0, 1, 2, 3), a0_ref, c0_ref)
        return carry

    lax.fori_loop(0, chunks // 2, two_others, 0)

    pressure = (ADIABATIC_INDEX - 1.0) * en_ref[...]
    density = density_ref[...] + deposit(0)
    rho_ref[...] = density
    lane = lax.broadcasted_iota(jnp.int32, (cx, cy, nz), 2)
    after = jnp.where(lane == nz - 1, 0.0, pltpu.roll(pressure, nz - 1, 2))
    before = jnp.where(lane == 0, 0.0, pltpu.roll(pressure, 1, 2))
    impulse_z = momentum_ref[2] + deposit(3) - KICK * (0.5 * (after - before))
    imp_ref[2] = impulse_z
    sound = jnp.sqrt(ADIABATIC_INDEX * pressure / density)
    wait_received(faces, range(4))
    low_x = jnp.where(gx > 0, in_face[0], 0.0)
    high_x = jnp.where(gx < n_gx - 1, in_face[1], 0.0)
    low_y = jnp.where(gy > 0, in_face[2] + own_ref[0], 0.0)
    high_y = jnp.where(gy < n_gy - 1, in_face[3] + own_ref[1], 0.0)
    after = jnp.concatenate([pressure[1:], high_x[None]], axis=0)
    before = jnp.concatenate([low_x[None], pressure[:-1]], axis=0)
    impulse_x = momentum_ref[0] + deposit(1) - KICK * (0.5 * (after - before))
    imp_ref[0] = impulse_x
    line = lax.broadcasted_iota(jnp.int32, (cx, cy, nz), 1)
    after = jnp.where(line == cy - 1, high_y[:, None, :], pltpu.roll(pressure, cy - 1, 1))
    before = jnp.where(line == 0, low_y[:, None, :], pltpu.roll(pressure, 1, 1))
    impulse_y = momentum_ref[1] + deposit(2) - KICK * (0.5 * (after - before))
    imp_ref[1] = impulse_y
    fastest = jnp.maximum(jnp.maximum(jnp.abs(impulse_x), jnp.abs(impulse_y)), jnp.abs(impulse_z))
    wave = fastest / density + sound

    def share_max(me, n, peer, slots, send, recv):
        copies = []
        for k in range(1, n):
            copies.append(pltpu.make_async_remote_copy(
                src_ref=slots.at[me], dst_ref=slots.at[me], send_sem=send.at[k],
                recv_sem=recv.at[k], device_id=peer(k), device_id_type=MESH,
            ))
        return copies

    top = jnp.max(jnp.max(wave, axis=0), axis=0, keepdims=True)
    max_p[plane] = jnp.maximum(top[:, 0:128], top[:, 128:256])
    to_hubs = []
    for n, spot in enumerate(HUBS):
        hub = spot[1] * n_gx + spot[0]
        to_hubs.append((jnp.logical_not(is_at((gx, gy), (spot,))), pltpu.make_async_remote_copy(
            src_ref=max_p.at[plane], dst_ref=max_h.at[lax.rem(me + devices - hub - 1, devices)], send_sem=mh_send.at[n],
            recv_sem=mh_recv.at[0], device_id={"gx": spot[0], "gy": spot[1]}, device_id_type=MESH,
        )))
    for other, copy in to_hubs:
        pl.when(other)(copy.start)
    sent_p = share_max(plane, half, plane_peer, max_p, mp_send, mp_recv)
    for copy in sent_p:
        copy.start()
    for copy in sent_p:
        copy.wait_recv()
    max_z[in_column] = jnp.max(max_p[...], axis=0)
    sent_z = share_max(in_column, n_column, column_peer, max_z, mz_send, mz_recv)
    for k in range(1, n_column):
        peer = column_peer(k)
        to_other = jnp.logical_not(is_at((peer["gx"], peer["gy"]), HUBS))
        pl.when(to_other)(sent_z[k - 1].start)

    @pl.when(not_hub)
    def _():
        for copy in sent_z:
            copy.wait_recv()
        step_ref[...] = COURANT / jnp.broadcast_to(jnp.max(max_z[...]), (1, 128))

    @pl.when(is_hub)
    def _():
        arrived = max_h.at[pl.ds(0, devices - 1)]
        pltpu.make_async_remote_copy(
            src_ref=arrived, dst_ref=arrived, send_sem=mh_send.at[0], recv_sem=mh_recv.at[0],
            device_id={"gx": HUBS[0][0], "gy": HUBS[0][1]}, device_id_type=MESH,
        ).wait_recv()
        best = jnp.maximum(jnp.max(arrived[...], axis=0), max_p[plane])
        step_ref[...] = COURANT / jnp.broadcast_to(jnp.max(best), (1, 128))

    for other, copy in to_hubs:
        pl.when(other)(copy.wait_send)
    for k in range(1, n_column):
        peer = column_peer(k)
        to_other = jnp.logical_not(is_at((peer["gx"], peer["gy"]), HUBS))
        pl.when(to_other)(sent_z[k - 1].wait_send)
    for copies in (moves, faces):
        for h in range(4):
            pl.when(inside[h])(copies[h].wait_send)
    for copy in sent_p:
        copy.wait_send()


def put_out(*refs):
    count = (len(refs) - 2) // 2
    step_ref, sem = refs[-2:]
    step_ref[0] = refs[count - 1][0, 0]
    copies = []
    for k in range(count):
        source = refs[k] if k < count - 1 else step_ref
        copy = pltpu.make_async_copy(source, refs[count + k], sem.at[k])
        copy.start()
        copies.append(copy)
    for copy in copies:
        copy.wait()


def on_device(n_gx, n_gy, density, momentum, energy, mass, velocity, temp, cell, count):
    rows = mass.shape[0]
    cap = rows // 16
    slots = rows + 4 * cap
    cx, cy, nz = density.shape
    vmem = pl.BlockSpec(memory_space=pltpu.VMEM)
    hbm = pl.BlockSpec(memory_space=pltpu.HBM)
    cells = cx * cy
    half = n_gy // 2
    dma = pltpu.SemaphoreType.DMA
    outs = pl.pallas_call(
        functools.partial(kernel, n_gx, n_gy),
        out_shape=(
            pltpu.VMEM(density.shape, F32),
            pltpu.VMEM(momentum.shape, F32),
            pltpu.VMEM(energy.shape, F32),
            pltpu.VMEM((5, slots), F32),
            pltpu.VMEM((3, slots), jnp.int32),
            pltpu.VMEM((1, 128), F32),
        ),
        in_specs=[hbm] * 8,
        out_specs=(vmem,) * 6,
        scratch_shapes=[
            pltpu.VMEM((8, rows), F32),
            pltpu.VMEM((8, rows), F32),
            pltpu.VMEM((1, rows), F32),
            pltpu.VMEM((1, rows), F32),
            pltpu.VMEM((1, rows), F32),
            pltpu.VMEM((4 * (cap // 128) * 16, CHUNK), BF16),
            pltpu.VMEM((4 * (cap // 128) * 16, CHUNK), BF16),
            pltpu.VMEM((128, CHUNK), BF16),
            pltpu.VMEM((128, CHUNK), BF16),
            pltpu.VMEM((4 * cells, CHUNK), BF16),
            pltpu.VMEM((4 * cells, CHUNK), BF16),
            pltpu.VMEM((4 * cells, CHUNK), F8),
            pltpu.VMEM((4 * cells, CHUNK), F8),
            pltpu.VMEM((cells, CHUNK), BF16),
            pltpu.VMEM((cells, CHUNK), BF16),
            pltpu.VMEM((cells, CHUNK), F8),
            pltpu.VMEM((cells, CHUNK), F8),
            pltpu.VMEM((nz, rows // 2), BF16),
            pltpu.VMEM((nz, rows // 2), BF16),
            pltpu.VMEM((nz, rows // 2), F8),
            pltpu.VMEM((nz, rows // 2), F8),
            pltpu.VMEM((5 * cells, nz), F32),
            pltpu.VMEM((5 * cells, nz), F32),
            pltpu.VMEM((4 * (cap // 128) * 16, 128), F32),
            pltpu.VMEM((4, 8, cap), F32),
            pltpu.VMEM((4, 8, cap), F32),
            pltpu.VMEM((4, cx, nz), F32),
            pltpu.VMEM((4, cx, nz), F32),
            pltpu.VMEM((2, cx, nz), F32),
            pltpu.VMEM((2 * n_gx, 1, 128), F32),
            pltpu.VMEM((half, 1, 128), F32),
            pltpu.VMEM((n_gx * n_gy, 1, 128), F32),
            dma((4,)),
            dma((4,)),
            dma((4,)),
            dma((4,)),
            dma((2 * n_gx,)),
            dma((2 * n_gx,)),
            dma((half,)),
            dma((half,)),
            dma((len(HUBS),)),
            dma((1,)),
            pltpu.VMEM((1, 1), jnp.int32),
            pltpu.VMEM(density.shape, F32),
            pltpu.VMEM(momentum.shape, F32),
            pltpu.VMEM(energy.shape, F32),
            pltpu.VMEM((1, rows), F32),
            pltpu.VMEM(velocity.shape, F32),
            pltpu.VMEM((1, rows), F32),
            pltpu.VMEM(cell.shape, jnp.int32),
            dma((8,)),
        ],
        compiler_params=pltpu.CompilerParams(
            collective_id=0, has_side_effects=True, vmem_limit_bytes=64200000
        ),
        name="spray",
    )(count.reshape(1, 1), density, momentum, energy, mass.reshape(1, rows), velocity, temp.reshape(1, rows), cell)
    final = pl.pallas_call(
        put_out,
        out_shape=tuple(pltpu.HBM(o.shape, o.dtype) for o in outs[:5]) + (pltpu.HBM((1,), F32),),
        in_specs=[vmem] * 6,
        out_specs=(hbm,) * 6,
        scratch_shapes=[pltpu.SMEM((1,), F32), dma((6,))],
        compiler_params=pltpu.CompilerParams(vmem_limit_bytes=8 * 1024 * 1024),
        name="put_out",
    )(*outs)
    return tuple(final[:5]) + (final[5].reshape(()),)


def solution(mesh):
    in_specs = (
        P("gx", "gy", None),
        P(None, "gx", "gy", None),
        P("gx", "gy", None),
        P(("gx", "gy")),
        P(None, ("gx", "gy")),
        P(("gx", "gy")),
        P(None, ("gx", "gy")),
        P(("gx", "gy")),
    )
    out_specs = (
        P("gx", "gy", None),
        P(None, "gx", "gy", None),
        P("gx", "gy", None),
        P(None, ("gx", "gy")),
        P(None, ("gx", "gy")),
        P(),
    )
    return jax.shard_map(
        functools.partial(on_device, mesh.shape["gx"], mesh.shape["gy"]),
        mesh=mesh, in_specs=in_specs, out_specs=out_specs, check_vma=False,
    )
```

```python
import functools

import jax
import jax.numpy as jnp
from jax import lax
from jax.experimental import pallas as pl
from jax.experimental.pallas import tpu as pltpu
from jax.sharding import PartitionSpec as P

ADIABATIC_INDEX = 1.4
KICK = 0.25
COURANT = 0.4
SHRINK = 0.5
MESH = pl.DeviceIdType.MESH
CHUNK = 1024
F32 = jnp.float32
BF16 = jnp.bfloat16
F8 = jnp.float8_e4m3fn
LIFT = 2048.0
HUBS = ((1, 0), (0, 1), (1, 1), (0, 4), (1, 4), (2, 0), (3, 0))


def dot_nt(a, b):
    return lax.dot_general(a, b, (((1,), (1,)), ((), ())), preferred_element_type=F32)


def two_terms(x):
    high = x.astype(BF16)
    low = (x - high.astype(F32)).astype(BF16)
    return high, low


def one_hot_rows(row, count):
    lanes = row.shape[1]
    base = (
        jnp.broadcast_to(row, (16, lanes))
        - lax.broadcasted_iota(jnp.int32, (16, lanes), 0).astype(F32)
    ).astype(BF16)
    one, zero = jnp.ones((16, lanes), BF16), jnp.zeros((16, lanes), BF16)
    return jnp.concatenate(
        [jnp.where(base == 16.0 * k, one, zero) for k in range(count // 16)], axis=0
    )


def kernel(
    n_gx, n_gy, count_hbm, density_hbm, momentum_hbm, energy_hbm, mass_hbm, vel_hbm, temp_hbm, cell_hbm,
    rho_ref, imp_ref, en_ref, state_ref, moved_ref, step_ref,
    src_ref, pay_ref, col_ref, q_ref, r_ref, g0_ref, g1_ref, h0_ref, h1_ref, a0_ref, a1_ref, c0_ref, c1_ref, e0_ref, e1_ref, f0_ref, f1_ref,
    b0_ref, b1_ref, d0_ref, d1_ref, acc_ref, low_ref, small_ref,
    out_bucket, in_bucket, out_face, in_face, own_ref, max_z, max_p, max_h,
    bucket_send, bucket_recv, face_send, face_recv, mz_send, mz_recv, mp_send, mp_recv, mh_send, mh_recv,
    count_ref, density_ref, momentum_ref, energy_ref, mass_ref, vel_ref, temp_ref, cell_ref, load_sem,
):
    sources = (count_hbm, mass_hbm, temp_hbm, vel_hbm, cell_hbm, energy_hbm, density_hbm, momentum_hbm)
    places = (count_ref, mass_ref, temp_ref, vel_ref, cell_ref, energy_ref, density_ref, momentum_ref)
    loads = []
    for k in range(8):
        load = pltpu.make_async_copy(sources[k], places[k], load_sem.at[k])
        load.start()
        loads.append(load)
    gx, gy = lax.axis_index("gx"), lax.axis_index("gy")
    cx, cy, nz = density_ref.shape
    rows = mass_ref.shape[1]
    cap = rows // 16
    per = cap // 128

    half = n_gy // 2
    upper_half, plane = gy // half, lax.rem(gy, half)
    in_column, n_column = upper_half * n_gx + gx, 2 * n_gx

    def column_peer(k):
        place = lax.rem(in_column + k, n_column)
        return {"gx": lax.rem(place, n_gx), "gy": place // n_gx * half + plane}

    def plane_peer(k):
        return {"gy": upper_half * half + lax.rem(plane + k, half)}

    targets = (
        {"gx": lax.rem(gx + n_gx - 1, n_gx)},
        {"gx": lax.rem(gx + 1, n_gx)},
        {"gy": lax.rem(gy + n_gy - 1, n_gy)},
        {"gy": lax.rem(gy + 1, n_gy)},
    )
    landing = (1, 0, 3, 2)

    barrier = pltpu.get_barrier_semaphore()
    greeted = [column_peer(k) for k in range(1, n_column)] + [plane_peer(k) for k in range(1, half)] + list(targets[2:])
    for peer in greeted:
        pl.semaphore_signal(barrier, inc=1, device_id=peer, device_id_type=MESH)

    devices = n_gx * n_gy

    def is_at(place, spots):
        found = jnp.bool_(False)
        for spot in spots:
            found = found | ((place[0] == spot[0]) & (place[1] == spot[1]))
        return found

    is_hub = is_at((gx, gy), HUBS)
    not_hub = jnp.logical_not(is_hub)
    me = gy * n_gx + gx

    @pl.when(is_hub)
    def _():
        def greet(j, carry):
            for k in range(15):
                other = lax.rem(j * 15 + k + me + 1, devices)
                peer = {"gx": lax.rem(other, n_gx), "gy": other // n_gx}
                pl.semaphore_signal(barrier, inc=1, device_id=peer, device_id_type=MESH)
            return carry

        lax.fori_loop(0, (devices - 1) // 15, greet, 0)

    for zeroed in (small_ref, acc_ref, low_ref):
        zeroed[...] = jnp.zeros_like(zeroed)
    for load in loads[:5]:
        load.wait()
    mass, temp = mass_ref[...], temp_ref[...]
    live = lax.broadcasted_iota(jnp.int32, (1, rows), 1) < jnp.broadcast_to(count_ref[...], (1, rows))
    evap = jnp.where(live, mass * jax.nn.sigmoid(2.0 * (temp - 2.0)), 0.0)
    vx, vy, vz = vel_ref[0:1, :], vel_ref[1:2, :], vel_ref[2:3, :]
    src_ref[0:1, :] = evap
    src_ref[1:2, :] = evap * vx
    src_ref[2:3, :] = evap * vy
    src_ref[3:4, :] = evap * vz
    src_ref[4:5, :] = evap * (temp + 0.5 * (vx * vx + vy * vy + vz * vz))
    pay_ref[0:1, :] = mass - SHRINK * evap
    pay_ref[1:4, :] = vel_ref[...]
    pay_ref[4:5, :] = temp
    pay_ref[5:8, :] = cell_ref[...].astype(F32)
    lx = cell_ref[0:1, :] - gx * cx
    ly = cell_ref[1:2, :] - gy * cy
    heading = jnp.where(
        lx < 0, 0, jnp.where(lx >= cx, 1, jnp.where(ly < 0, 2, jnp.where(ly >= cy, 3, 4)))
    )
    heading = jnp.where(live, heading, 5)
    stays = heading == 4
    col_ref[...] = jnp.where(stays, lx * cy + ly, -1000).astype(F32)
    state_ref[:, :rows] = jnp.where(stays, pay_ref[0:5, :], 0.0)
    moved_ref[:, :rows] = jnp.where(stays, cell_ref[...], 0)

    blocks = rows // 128
    marks = jnp.where(
        jnp.broadcast_to(heading, (8, rows)) == lax.broadcasted_iota(jnp.int32, (8, rows), 0), 1.0, 0.0
    )
    stacked = jnp.concatenate([marks[:, k * 128 : (k + 1) * 128] for k in range(blocks)], axis=0)
    i0 = lax.broadcasted_iota(jnp.int32, (128, 256), 0)
    i1 = lax.broadcasted_iota(jnp.int32, (128, 256), 1)
    upper = jnp.where((i0 < i1) | (i1 >= 128), 1.0, 0.0).astype(BF16)
    sums = jnp.dot(stacked.astype(BF16), upper, preferred_element_type=F32)
    carry = jnp.zeros((8, 128), F32)
    ranks = []
    for k in range(blocks):
        part = sums[k * 8 : (k + 1) * 8]
        mark = stacked[k * 8 : (k + 1) * 8]
        ranks.append(jnp.sum((part[:, :128] + carry) * mark, axis=0, keepdims=True))
        carry = carry + part[:, 128:]
    rank = jnp.concatenate(ranks, axis=1).astype(jnp.int32)
    q_ref[...] = jnp.where(heading < 4, heading * per + (rank >> 7), -1).astype(F32)
    r_ref[...] = (rank & 127).astype(F32)

    inside = (gx > 0, gx < n_gx - 1, gy > 0, gy < n_gy - 1)

    def exchange(src, dst, send, recv):
        copies = []
        for h in range(4):
            copy = pltpu.make_async_remote_copy(
                src_ref=src.at[h], dst_ref=dst.at[landing[h]], send_sem=send.at[h],
                recv_sem=recv.at[landing[h]], device_id=targets[h], device_id_type=MESH,
            )
            copies.append(copy)
        return copies

    def send(copies, which):
        for h in which:
            pl.when(inside[h])(copies[h].start)

    def wait_received(copies, which):
        for h in which:
            pl.when(inside[landing[h]])(copies[h].wait_recv)

    for b in range(4):
        @pl.when(jnp.logical_not(inside[b]))
        def _():
            in_bucket[b] = jnp.zeros(in_bucket.shape[1:], F32)

    cells = cx * cy
    chunks = rows // CHUNK
    groups = 4 * per

    def spread(lanes, values, a_ref, c_ref):
        base = (
            jnp.broadcast_to(col_ref[:, lanes], (16, CHUNK))
            - lax.broadcasted_iota(jnp.int32, (16, CHUNK), 0).astype(F32)
        ).astype(BF16)
        zero = jnp.zeros((16, CHUNK), BF16)
        hits = [base == 16.0 * k for k in range(cells // 16)]
        for n, v in enumerate(values):
            value = jnp.broadcast_to(src_ref[v : v + 1, lanes], (16, CHUNK))
            high = value.astype(BF16)
            low = ((value - high.astype(F32)) * LIFT).astype(BF16)
            for k in range(cells // 16):
                at = n * cells + k * 16
                a_ref[at : at + 16, :] = jnp.where(hits[k], high, zero)
            for k in range(0, cells // 16, 2):
                at = n * cells + k * 16
                pair = jnp.concatenate([jnp.where(hits[k], low, zero), jnp.where(hits[k + 1], low, zero)], axis=0)
                c_ref[at : at + 32, :] = pair.astype(F8)

    def chunk_of(c):
        if isinstance(c, int):
            return slice(c * CHUNK, (c + 1) * CHUNK)
        return pl.ds(pl.multiple_of(c * CHUNK, CHUNK), CHUNK)

    def build_pack(c, g_ref, h_ref):
        lanes = chunk_of(c)
        high, low = two_terms(pay_ref[:, lanes])
        both = jnp.concatenate([high.astype(F32), low.astype(F32)], axis=0).astype(BF16)
        q = jnp.broadcast_to(q_ref[:, lanes], (16, CHUNK)).astype(BF16)
        zero = jnp.zeros((16, CHUNK), BF16)
        for k in range(groups):
            g_ref[k * 16 : (k + 1) * 16, :] = jnp.where(q == float(k), both, zero)
        h_ref[...] = one_hot_rows(r_ref[:, lanes], 128)

    build_pack(0, g0_ref, h0_ref)

    moves = exchange(out_bucket, in_bucket, bucket_send, bucket_recv)
    faces = exchange(out_face, in_face, face_send, face_recv)

    e_rows = slice(4 * cells, 5 * cells)

    def build_energy(c, i, a_ref, c_ref, b_ref, d_ref):
        lanes, place = chunk_of(c), chunk_of(i)
        spread(lanes, (4,), a_ref, c_ref)
        depth = one_hot_rows(cell_ref[2:3, lanes].astype(F32), nz)
        b_ref[:, place] = depth
        d_ref[:, place] = depth.astype(F8)

    build_energy(0, 0, e0_ref, f0_ref, b0_ref, d0_ref)

    def send_moves():
        pl.when(is_hub)(lambda: pl.semaphore_wait(barrier, len(greeted) + len(HUBS) - 1))
        pl.when(not_hub)(lambda: pl.semaphore_wait(barrier, len(greeted) + len(HUBS)))
        send(moves, (2, 3, 0, 1))

    def two_energy(i, carry):
        place = chunk_of(i)
        acc_ref[e_rows, :] += dot_nt(e0_ref[...], b0_ref[:, place])
        low_ref[e_rows, :] += dot_nt(f0_ref[...], d0_ref[:, place])
        small_ref[...] += dot_nt(g0_ref[...], h0_ref[...])
        build_energy(2 * i + 1, i, e1_ref, f1_ref, b1_ref, d1_ref)
        build_pack(2 * i + 1, g1_ref, h1_ref)
        acc_ref[e_rows, :] += dot_nt(e1_ref[...], b1_ref[:, place])
        low_ref[e_rows, :] += dot_nt(f1_ref[...], d1_ref[:, place])
        small_ref[...] += dot_nt(g1_ref[...], h1_ref[...])
        later = jnp.minimum(i + 1, chunks // 2 - 1)
        build_energy(2 * later, later, e0_ref, f0_ref, b0_ref, d0_ref)
        build_pack(2 * later, g0_ref, h0_ref)
        return carry

    lax.fori_loop(0, chunks // 4, lambda i, carry: two_energy(2 * i + 1, two_energy(2 * i, carry)), 0)
    for h in range(4):
        for j in range(per):
            k = (h * per + j) * 16
            out_bucket[h, :, j * 128 : (j + 1) * 128] = small_ref[k : k + 8, :] + small_ref[k + 8 : k + 16, :]
    send_moves()

    def sums_of(got, b, with_all):
        warm = got[4:5]
        share = jax.nn.sigmoid(2.0 * (warm - 2.0))
        boiled = got[0:1] * share / (1.0 - SHRINK * share)
        speed = got[1:4]
        budget = 0.5 * jnp.sum(speed * speed, axis=0, keepdims=True)
        values = [boiled * (warm + budget)]
        if with_all:
            values = [boiled] + [boiled * got[k : k + 1] for k in (1, 2, 3)] + values
        if b < 2:
            along = got[6:7] - (gy * cy).astype(F32)
        else:
            along = got[5:6] - (gx * cx).astype(F32)
        hit = (
            jnp.broadcast_to(along, (16, cap))
            == lax.broadcasted_iota(jnp.int32, (16, cap), 0).astype(F32)
        )
        parts = []
        for value in values:
            wide = jnp.where(hit, jnp.broadcast_to(value, (16, cap)), 0.0)
            parts.append(two_terms(wide))
        left = jnp.concatenate([p[0] for p in parts] + [p[1] for p in parts], axis=0)
        sums = dot_nt(left, one_hot_rows(got[7:8], nz))
        n = len(values) * 16
        return sums[0:n] + sums[n : 2 * n]

    def receive(b):
        got = in_bucket[b]
        state_ref[:, rows + b * cap : rows + (b + 1) * cap] = got[0:5]
        moved_ref[:, rows + b * cap : rows + (b + 1) * cap] = got[5:8].astype(jnp.int32)
        sums = sums_of(got, b, True)
        for v in range(5):
            part = sums[v * 16 : (v + 1) * 16]
            if b < 2:
                at = v * cells + (0 if b == 0 else (cx - 1) * cy)
                acc_ref[at : at + cy, :] += part
            else:
                edge = 0 if b == 2 else cy - 1
                for x in range(cx):
                    at = v * cells + x * cy + edge
                    acc_ref[at : at + 1, :] += part[x : x + 1]

    def deposit(v):
        at = slice(v * cells, (v + 1) * cells)
        return (acc_ref[at, :] + low_ref[at, :] * (1.0 / LIFT)).reshape(cx, cy, nz)

    def receive_x():
        wait_received(moves, (0, 1))
        receive(0)
        receive(1)
        for load in loads[5:]:
            load.wait()
        energy = energy_ref[...] + deposit(4)
        for x in range(cx):
            out_face[2, x : x + 1, :] = (ADIABATIC_INDEX - 1.0) * energy[x, 0:1, :]
            out_face[3, x : x + 1, :] = (ADIABATIC_INDEX - 1.0) * energy[x, cy - 1 : cy, :]
        send(faces, (2, 3))

    def receive_y():
        wait_received(moves, (2, 3))
        receive(2)
        receive(3)
        for h in (2, 3):
            own_ref[h - 2] = (ADIABATIC_INDEX - 1.0) * sums_of(out_bucket[h], h, False)
        energy = energy_ref[...] + deposit(4)
        en_ref[...] = energy
        out_face[0] = (ADIABATIC_INDEX - 1.0) * energy[0]
        out_face[1] = (ADIABATIC_INDEX - 1.0) * energy[cx - 1]
        send(faces, (0, 1))

    far = (gy == half - 1) | (gy == half)
    others = slice(0, 4 * cells)
    spread(chunk_of(0), (0, 1, 2, 3), a0_ref, c0_ref)

    def two_others(i, carry):
        pl.when(i == 1)(receive_x)
        pl.when(((i == 2) & jnp.logical_not(far)) | ((i == 3) & far))(receive_y)
        place = chunk_of(i)
        acc_ref[others, :] += dot_nt(a0_ref[...], b0_ref[:, place])
        low_ref[others, :] += dot_nt(c0_ref[...], d0_ref[:, place])
        spread(chunk_of(2 * i + 1), (0, 1, 2, 3), a1_ref, c1_ref)
        acc_ref[others, :] += dot_nt(a1_ref[...], b1_ref[:, place])
        low_ref[others, :] += dot_nt(c1_ref[...], d1_ref[:, place])
        spread(chunk_of(jnp.minimum(2 * i + 2, chunks - 1)), (0, 1, 2, 3), a0_ref, c0_ref)
        return carry

    lax.fori_loop(0, chunks // 2, two_others, 0)

    pressure = (ADIABATIC_INDEX - 1.0) * en_ref[...]
    density = density_ref[...] + deposit(0)
    rho_ref[...] = density
    lane = lax.broadcasted_iota(jnp.int32, (cx, cy, nz), 2)
    after = jnp.where(lane == nz - 1, 0.0, pltpu.roll(pressure, nz - 1, 2))
    before = jnp.where(lane == 0, 0.0, pltpu.roll(pressure, 1, 2))
    impulse_z = momentum_ref[2] + deposit(3) - KICK * (0.5 * (after - before))
    imp_ref[2] = impulse_z
    sound = jnp.sqrt(ADIABATIC_INDEX * pressure / density)
    wait_received(faces, range(4))
    low_x = jnp.where(gx > 0, in_face[0], 0.0)
    high_x = jnp.where(gx < n_gx - 1, in_face[1], 0.0)
    low_y = jnp.where(gy > 0, in_face[2] + own_ref[0], 0.0)
    high_y = jnp.where(gy < n_gy - 1, in_face[3] + own_ref[1], 0.0)
    after = jnp.concatenate([pressure[1:], high_x[None]], axis=0)
    before = jnp.concatenate([low_x[None], pressure[:-1]], axis=0)
    impulse_x = momentum_ref[0] + deposit(1) - KICK * (0.5 * (after - before))
    imp_ref[0] = impulse_x
    line = lax.broadcasted_iota(jnp.int32, (cx, cy, nz), 1)
    after = jnp.where(line == cy - 1, high_y[:, None, :], pltpu.roll(pressure, cy - 1, 1))
    before = jnp.where(line == 0, low_y[:, None, :], pltpu.roll(pressure, 1, 1))
    impulse_y = momentum_ref[1] + deposit(2) - KICK * (0.5 * (after - before))
    imp_ref[1] = impulse_y
    fastest = jnp.maximum(jnp.maximum(jnp.abs(impulse_x), jnp.abs(impulse_y)), jnp.abs(impulse_z))
    wave = fastest / density + sound

    def share_max(me, n, peer, slots, send, recv):
        copies = []
        for k in range(1, n):
            copies.append(pltpu.make_async_remote_copy(
                src_ref=slots.at[me], dst_ref=slots.at[me], send_sem=send.at[k],
                recv_sem=recv.at[k], device_id=peer(k), device_id_type=MESH,
            ))
        return copies

    top = jnp.max(jnp.max(wave, axis=0), axis=0, keepdims=True)
    max_p[plane] = jnp.maximum(top[:, 0:128], top[:, 128:256])
    to_hubs = []
    for n, spot in enumerate(HUBS):
        hub = spot[1] * n_gx + spot[0]
        to_hubs.append((jnp.logical_not(is_at((gx, gy), (spot,))), pltpu.make_async_remote_copy(
            src_ref=max_p.at[plane], dst_ref=max_h.at[lax.rem(me + devices - hub - 1, devices)], send_sem=mh_send.at[n],
            recv_sem=mh_recv.at[0], device_id={"gx": spot[0], "gy": spot[1]}, device_id_type=MESH,
        )))
    for other, copy in to_hubs:
        pl.when(other)(copy.start)
    sent_p = share_max(plane, half, plane_peer, max_p, mp_send, mp_recv)
    for copy in sent_p:
        copy.start()
    for copy in sent_p:
        copy.wait_recv()
    max_z[in_column] = jnp.max(max_p[...], axis=0)
    sent_z = share_max(in_column, n_column, column_peer, max_z, mz_send, mz_recv)
    for k in range(1, n_column):
        peer = column_peer(k)
        to_other = jnp.logical_not(is_at((peer["gx"], peer["gy"]), HUBS))
        pl.when(to_other)(sent_z[k - 1].start)

    @pl.when(not_hub)
    def _():
        for copy in sent_z:
            copy.wait_recv()
        step_ref[...] = COURANT / jnp.broadcast_to(jnp.max(max_z[...]), (1, 128))

    @pl.when(is_hub)
    def _():
        arrived = max_h.at[pl.ds(0, devices - 1)]
        pltpu.make_async_remote_copy(
            src_ref=arrived, dst_ref=arrived, send_sem=mh_send.at[0], recv_sem=mh_recv.at[0],
            device_id={"gx": HUBS[0][0], "gy": HUBS[0][1]}, device_id_type=MESH,
        ).wait_recv()
        best = jnp.maximum(jnp.max(arrived[...], axis=0), max_p[plane])
        step_ref[...] = COURANT / jnp.broadcast_to(jnp.max(best), (1, 128))

    for other, copy in to_hubs:
        pl.when(other)(copy.wait_send)
    for k in range(1, n_column):
        peer = column_peer(k)
        to_other = jnp.logical_not(is_at((peer["gx"], peer["gy"]), HUBS))
        pl.when(to_other)(sent_z[k - 1].wait_send)
    for copies in (moves, faces):
        for h in range(4):
            pl.when(inside[h])(copies[h].wait_send)
    for copy in sent_p:
        copy.wait_send()


def put_out(*refs):
    count = (len(refs) - 2) // 2
    step_ref, sem = refs[-2:]
    step_ref[0] = refs[count - 1][0, 0]
    copies = []
    for k in range(count):
        source = refs[k] if k < count - 1 else step_ref
        copy = pltpu.make_async_copy(source, refs[count + k], sem.at[k])
        copy.start()
        copies.append(copy)
    for copy in copies:
        copy.wait()


def on_device(n_gx, n_gy, density, momentum, energy, mass, velocity, temp, cell, count):
    rows = mass.shape[0]
    cap = rows // 16
    slots = rows + 4 * cap
    cx, cy, nz = density.shape
    vmem = pl.BlockSpec(memory_space=pltpu.VMEM)
    hbm = pl.BlockSpec(memory_space=pltpu.HBM)
    cells = cx * cy
    half = n_gy // 2
    dma = pltpu.SemaphoreType.DMA
    outs = pl.pallas_call(
        functools.partial(kernel, n_gx, n_gy),
        out_shape=(
            pltpu.VMEM(density.shape, F32),
            pltpu.VMEM(momentum.shape, F32),
            pltpu.VMEM(energy.shape, F32),
            pltpu.VMEM((5, slots), F32),
            pltpu.VMEM((3, slots), jnp.int32),
            pltpu.VMEM((1, 128), F32),
        ),
        in_specs=[hbm] * 8,
        out_specs=(vmem,) * 6,
        scratch_shapes=[
            pltpu.VMEM((8, rows), F32),
            pltpu.VMEM((8, rows), F32),
            pltpu.VMEM((1, rows), F32),
            pltpu.VMEM((1, rows), F32),
            pltpu.VMEM((1, rows), F32),
            pltpu.VMEM((4 * (cap // 128) * 16, CHUNK), BF16),
            pltpu.VMEM((4 * (cap // 128) * 16, CHUNK), BF16),
            pltpu.VMEM((128, CHUNK), BF16),
            pltpu.VMEM((128, CHUNK), BF16),
            pltpu.VMEM((4 * cells, CHUNK), BF16),
            pltpu.VMEM((4 * cells, CHUNK), BF16),
            pltpu.VMEM((4 * cells, CHUNK), F8),
            pltpu.VMEM((4 * cells, CHUNK), F8),
            pltpu.VMEM((cells, CHUNK), BF16),
            pltpu.VMEM((cells, CHUNK), BF16),
            pltpu.VMEM((cells, CHUNK), F8),
            pltpu.VMEM((cells, CHUNK), F8),
            pltpu.VMEM((nz, rows // 2), BF16),
            pltpu.VMEM((nz, rows // 2), BF16),
            pltpu.VMEM((nz, rows // 2), F8),
            pltpu.VMEM((nz, rows // 2), F8),
            pltpu.VMEM((5 * cells, nz), F32),
            pltpu.VMEM((5 * cells, nz), F32),
            pltpu.VMEM((4 * (cap // 128) * 16, 128), F32),
            pltpu.VMEM((4, 8, cap), F32),
            pltpu.VMEM((4, 8, cap), F32),
            pltpu.VMEM((4, cx, nz), F32),
            pltpu.VMEM((4, cx, nz), F32),
            pltpu.VMEM((2, cx, nz), F32),
            pltpu.VMEM((2 * n_gx, 1, 128), F32),
            pltpu.VMEM((half, 1, 128), F32),
            pltpu.VMEM((n_gx * n_gy, 1, 128), F32),
            dma((4,)),
            dma((4,)),
            dma((4,)),
            dma((4,)),
            dma((2 * n_gx,)),
            dma((2 * n_gx,)),
            dma((half,)),
            dma((half,)),
            dma((len(HUBS),)),
            dma((1,)),
            pltpu.VMEM((1, 1), jnp.int32),
            pltpu.VMEM(density.shape, F32),
            pltpu.VMEM(momentum.shape, F32),
            pltpu.VMEM(energy.shape, F32),
            pltpu.VMEM((1, rows), F32),
            pltpu.VMEM(velocity.shape, F32),
            pltpu.VMEM((1, rows), F32),
            pltpu.VMEM(cell.shape, jnp.int32),
            dma((8,)),
        ],
        compiler_params=pltpu.CompilerParams(
            collective_id=0, has_side_effects=True, vmem_limit_bytes=64200000
        ),
        name="spray",
    )(count.reshape(1, 1), density, momentum, energy, mass.reshape(1, rows), velocity, temp.reshape(1, rows), cell)
    final = pl.pallas_call(
        put_out,
        out_shape=tuple(pltpu.HBM(o.shape, o.dtype) for o in outs[:5]) + (pltpu.HBM((1,), F32),),
        in_specs=[vmem] * 6,
        out_specs=(hbm,) * 6,
        scratch_shapes=[pltpu.SMEM((1,), F32), dma((6,))],
        compiler_params=pltpu.CompilerParams(vmem_limit_bytes=8 * 1024 * 1024),
        name="put_out",
    )(*outs)
    return tuple(final[:5]) + (final[5].reshape(()),)


def solution(mesh):
    in_specs = (
        P("gx", "gy", None),
        P(None, "gx", "gy", None),
        P("gx", "gy", None),
        P(("gx", "gy")),
        P(None, ("gx", "gy")),
        P(("gx", "gy")),
        P(None, ("gx", "gy")),
        P(("gx", "gy")),
    )
    out_specs = (
        P("gx", "gy", None),
        P(None, "gx", "gy", None),
        P("gx", "gy", None),
        P(None, ("gx", "gy")),
        P(None, ("gx", "gy")),
        P(),
    )
    return jax.shard_map(
        functools.partial(on_device, mesh.shape["gx"], mesh.shape["gy"]),
        mesh=mesh, in_specs=in_specs, out_specs=out_specs, check_vma=False,
    )
```

```python
import functools

import jax
import jax.numpy as jnp
from jax import lax
from jax.experimental import pallas as pl
from jax.experimental.pallas import tpu as pltpu
from jax.sharding import PartitionSpec as P

ADIABATIC_INDEX = 1.4
KICK = 0.25
COURANT = 0.4
SHRINK = 0.5
MESH = pl.DeviceIdType.MESH
CHUNK = 1024
F32 = jnp.float32
BF16 = jnp.bfloat16
F8 = jnp.float8_e4m3fn
LIFT = 2048.0
HUBS = ((1, 0), (0, 1), (1, 1), (0, 4), (1, 4), (2, 0), (3, 0))


def dot_nt(a, b):
    return lax.dot_general(a, b, (((1,), (1,)), ((), ())), preferred_element_type=F32)


def two_terms(x):
    high = x.astype(BF16)
    low = (x - high.astype(F32)).astype(BF16)
    return high, low


def one_hot_rows(row, count):
    lanes = row.shape[1]
    base = (
        jnp.broadcast_to(row, (16, lanes))
        - lax.broadcasted_iota(jnp.int32, (16, lanes), 0).astype(F32)
    ).astype(BF16)
    one, zero = jnp.ones((16, lanes), BF16), jnp.zeros((16, lanes), BF16)
    return jnp.concatenate(
        [jnp.where(base == 16.0 * k, one, zero) for k in range(count // 16)], axis=0
    )


def kernel(
    n_gx, n_gy, count_hbm, density_hbm, momentum_hbm, energy_hbm, mass_hbm, vel_hbm, temp_hbm, cell_hbm,
    rho_ref, imp_ref, en_ref, state_ref, moved_ref, step_ref,
    src_ref, pay_ref, col_ref, q_ref, r_ref, g0_ref, g1_ref, h0_ref, h1_ref, a0_ref, a1_ref, c0_ref, c1_ref, e0_ref, e1_ref, f0_ref, f1_ref,
    b0_ref, b1_ref, d0_ref, d1_ref, acc_ref, low_ref, small_ref,
    out_bucket, in_bucket, out_face, in_face, own_ref, max_z, max_p, max_h,
    bucket_send, bucket_recv, face_send, face_recv, mz_send, mz_recv, mp_send, mp_recv, mh_send, mh_recv,
    count_ref, density_ref, momentum_ref, energy_ref, mass_ref, vel_ref, temp_ref, cell_ref, load_sem,
):
    sources = (count_hbm, mass_hbm, temp_hbm, vel_hbm, cell_hbm, energy_hbm, density_hbm, momentum_hbm)
    places = (count_ref, mass_ref, temp_ref, vel_ref, cell_ref, energy_ref, density_ref, momentum_ref)
    loads = []
    for k in range(8):
        load = pltpu.make_async_copy(sources[k], places[k], load_sem.at[k])
        load.start()
        loads.append(load)
    gx, gy = lax.axis_index("gx"), lax.axis_index("gy")
    cx, cy, nz = density_ref.shape
    rows = mass_ref.shape[1]
    cap = rows // 16
    per = cap // 128

    half = n_gy // 2
    upper_half, plane = gy // half, lax.rem(gy, half)
    in_column, n_column = upper_half * n_gx + gx, 2 * n_gx

    def column_peer(k):
        place = lax.rem(in_column + k, n_column)
        return {"gx": lax.rem(place, n_gx), "gy": place // n_gx * half + plane}

    def plane_peer(k):
        return {"gy": upper_half * half + lax.rem(plane + k, half)}

    targets = (
        {"gx": lax.rem(gx + n_gx - 1, n_gx)},
        {"gx": lax.rem(gx + 1, n_gx)},
        {"gy": lax.rem(gy + n_gy - 1, n_gy)},
        {"gy": lax.rem(gy + 1, n_gy)},
    )
    landing = (1, 0, 3, 2)

    barrier = pltpu.get_barrier_semaphore()
    greeted = [column_peer(k) for k in range(1, n_column)] + [plane_peer(k) for k in range(1, half)] + list(targets[2:])
    for peer in greeted:
        pl.semaphore_signal(barrier, inc=1, device_id=peer, device_id_type=MESH)

    devices = n_gx * n_gy

    def is_at(place, spots):
        found = jnp.bool_(False)
        for spot in spots:
            found = found | ((place[0] == spot[0]) & (place[1] == spot[1]))
        return found

    is_hub = is_at((gx, gy), HUBS)
    not_hub = jnp.logical_not(is_hub)
    me = gy * n_gx + gx

    @pl.when(is_hub)
    def _():
        def greet(j, carry):
            for k in range(15):
                other = lax.rem(j * 15 + k + me + 1, devices)
                peer = {"gx": lax.rem(other, n_gx), "gy": other // n_gx}
                pl.semaphore_signal(barrier, inc=1, device_id=peer, device_id_type=MESH)
            return carry

        lax.fori_loop(0, (devices - 1) // 15, greet, 0)

    for zeroed in (small_ref, acc_ref, low_ref):
        zeroed[...] = jnp.zeros_like(zeroed)
    for load in loads[:5]:
        load.wait()
    mass, temp = mass_ref[...], temp_ref[...]
    live = lax.broadcasted_iota(jnp.int32, (1, rows), 1) < jnp.broadcast_to(count_ref[...], (1, rows))
    evap = jnp.where(live, mass * jax.nn.sigmoid(2.0 * (temp - 2.0)), 0.0)
    vx, vy, vz = vel_ref[0:1, :], vel_ref[1:2, :], vel_ref[2:3, :]
    src_ref[0:1, :] = evap
    src_ref[1:2, :] = evap * vx
    src_ref[2:3, :] = evap * vy
    src_ref[3:4, :] = evap * vz
    src_ref[4:5, :] = evap * (temp + 0.5 * (vx * vx + vy * vy + vz * vz))
    pay_ref[0:1, :] = mass - SHRINK * evap
    pay_ref[1:4, :] = vel_ref[...]
    pay_ref[4:5, :] = temp
    pay_ref[5:8, :] = cell_ref[...].astype(F32)
    lx = cell_ref[0:1, :] - gx * cx
    ly = cell_ref[1:2, :] - gy * cy
    heading = jnp.where(
        lx < 0, 0, jnp.where(lx >= cx, 1, jnp.where(ly < 0, 2, jnp.where(ly >= cy, 3, 4)))
    )
    heading = jnp.where(live, heading, 5)
    stays = heading == 4
    col_ref[...] = jnp.where(stays, lx * cy + ly, -1000).astype(F32)

    blocks = rows // 128
    marks = jnp.where(
        jnp.broadcast_to(heading, (8, rows)) == lax.broadcasted_iota(jnp.int32, (8, rows), 0), 1.0, 0.0
    )
    stacked = jnp.concatenate([marks[:, k * 128 : (k + 1) * 128] for k in range(blocks)], axis=0)
    i0 = lax.broadcasted_iota(jnp.int32, (128, 256), 0)
    i1 = lax.broadcasted_iota(jnp.int32, (128, 256), 1)
    upper = jnp.where((i0 < i1) | (i1 >= 128), 1.0, 0.0).astype(BF16)
    sums = jnp.dot(stacked.astype(BF16), upper, preferred_element_type=F32)
    carry = jnp.zeros((8, 128), F32)
    ranks = []
    for k in range(blocks):
        part = sums[k * 8 : (k + 1) * 8]
        mark = stacked[k * 8 : (k + 1) * 8]
        ranks.append(jnp.sum((part[:, :128] + carry) * mark, axis=0, keepdims=True))
        carry = carry + part[:, 128:]
    rank = jnp.concatenate(ranks, axis=1).astype(jnp.int32)
    q_ref[...] = jnp.where(heading < 4, heading * per + (rank >> 7), -1).astype(F32)
    r_ref[...] = (rank & 127).astype(F32)

    inside = (gx > 0, gx < n_gx - 1, gy > 0, gy < n_gy - 1)

    def exchange(src, dst, send, recv):
        copies = []
        for h in range(4):
            copy = pltpu.make_async_remote_copy(
                src_ref=src.at[h], dst_ref=dst.at[landing[h]], send_sem=send.at[h],
                recv_sem=recv.at[landing[h]], device_id=targets[h], device_id_type=MESH,
            )
            copies.append(copy)
        return copies

    def send(copies, which):
        for h in which:
            pl.when(inside[h])(copies[h].start)

    def wait_received(copies, which):
        for h in which:
            pl.when(inside[landing[h]])(copies[h].wait_recv)

    for b in range(4):
        @pl.when(jnp.logical_not(inside[b]))
        def _():
            in_bucket[b] = jnp.zeros(in_bucket.shape[1:], F32)

    cells = cx * cy
    chunks = rows // CHUNK
    groups = 4 * per

    def spread(lanes, values, a_ref, c_ref):
        base = (
            jnp.broadcast_to(col_ref[:, lanes], (16, CHUNK))
            - lax.broadcasted_iota(jnp.int32, (16, CHUNK), 0).astype(F32)
        ).astype(BF16)
        zero = jnp.zeros((16, CHUNK), BF16)
        hits = [base == 16.0 * k for k in range(cells // 16)]
        for n, v in enumerate(values):
            value = jnp.broadcast_to(src_ref[v : v + 1, lanes], (16, CHUNK))
            high = value.astype(BF16)
            low = ((value - high.astype(F32)) * LIFT).astype(BF16)
            for k in range(cells // 16):
                at = n * cells + k * 16
                a_ref[at : at + 16, :] = jnp.where(hits[k], high, zero)
            for k in range(0, cells // 16, 2):
                at = n * cells + k * 16
                pair = jnp.concatenate([jnp.where(hits[k], low, zero), jnp.where(hits[k + 1], low, zero)], axis=0)
                c_ref[at : at + 32, :] = pair.astype(F8)

    def chunk_of(c):
        if isinstance(c, int):
            return slice(c * CHUNK, (c + 1) * CHUNK)
        return pl.ds(pl.multiple_of(c * CHUNK, CHUNK), CHUNK)

    def build_pack(c, g_ref, h_ref):
        lanes = chunk_of(c)
        high, low = two_terms(pay_ref[:, lanes])
        both = jnp.concatenate([high.astype(F32), low.astype(F32)], axis=0).astype(BF16)
        q = jnp.broadcast_to(q_ref[:, lanes], (16, CHUNK)).astype(BF16)
        zero = jnp.zeros((16, CHUNK), BF16)
        for k in range(groups):
            g_ref[k * 16 : (k + 1) * 16, :] = jnp.where(q == float(k), both, zero)
        h_ref[...] = one_hot_rows(r_ref[:, lanes], 128)

    build_pack(0, g0_ref, h0_ref)

    moves = exchange(out_bucket, in_bucket, bucket_send, bucket_recv)
    faces = exchange(out_face, in_face, face_send, face_recv)

    e_rows = slice(4 * cells, 5 * cells)

    def build_energy(c, i, a_ref, c_ref, b_ref, d_ref):
        lanes, place = chunk_of(c), chunk_of(i)
        spread(lanes, (4,), a_ref, c_ref)
        depth = one_hot_rows(cell_ref[2:3, lanes].astype(F32), nz)
        b_ref[:, place] = depth
        d_ref[:, place] = depth.astype(F8)

    build_energy(0, 0, e0_ref, f0_ref, b0_ref, d0_ref)

    def send_moves():
        pl.when(is_hub)(lambda: pl.semaphore_wait(barrier, len(greeted) + len(HUBS) - 1))
        pl.when(not_hub)(lambda: pl.semaphore_wait(barrier, len(greeted) + len(HUBS)))
        send(moves, (2, 3, 0, 1))

    def two_energy(i, carry):
        place = chunk_of(i)
        acc_ref[e_rows, :] += dot_nt(e0_ref[...], b0_ref[:, place])
        low_ref[e_rows, :] += dot_nt(f0_ref[...], d0_ref[:, place])
        small_ref[...] += dot_nt(g0_ref[...], h0_ref[...])
        build_energy(2 * i + 1, i, e1_ref, f1_ref, b1_ref, d1_ref)
        build_pack(2 * i + 1, g1_ref, h1_ref)
        acc_ref[e_rows, :] += dot_nt(e1_ref[...], b1_ref[:, place])
        low_ref[e_rows, :] += dot_nt(f1_ref[...], d1_ref[:, place])
        small_ref[...] += dot_nt(g1_ref[...], h1_ref[...])
        later = jnp.minimum(i + 1, chunks // 2 - 1)
        build_energy(2 * later, later, e0_ref, f0_ref, b0_ref, d0_ref)
        build_pack(2 * later, g0_ref, h0_ref)
        return carry

    lax.fori_loop(0, chunks // 4, lambda i, carry: two_energy(2 * i + 1, two_energy(2 * i, carry)), 0)
    for h in range(4):
        for j in range(per):
            k = (h * per + j) * 16
            out_bucket[h, :, j * 128 : (j + 1) * 128] = small_ref[k : k + 8, :] + small_ref[k + 8 : k + 16, :]
    send_moves()

    def sums_of(got, b, with_all):
        warm = got[4:5]
        share = jax.nn.sigmoid(2.0 * (warm - 2.0))
        boiled = got[0:1] * share / (1.0 - SHRINK * share)
        speed = got[1:4]
        budget = 0.5 * jnp.sum(speed * speed, axis=0, keepdims=True)
        values = [boiled * (warm + budget)]
        if with_all:
            values = [boiled] + [boiled * got[k : k + 1] for k in (1, 2, 3)] + values
        if b < 2:
            along = got[6:7] - (gy * cy).astype(F32)
        else:
            along = got[5:6] - (gx * cx).astype(F32)
        hit = (
            jnp.broadcast_to(along, (16, cap))
            == lax.broadcasted_iota(jnp.int32, (16, cap), 0).astype(F32)
        )
        parts = []
        for value in values:
            wide = jnp.where(hit, jnp.broadcast_to(value, (16, cap)), 0.0)
            parts.append(two_terms(wide))
        left = jnp.concatenate([p[0] for p in parts] + [p[1] for p in parts], axis=0)
        sums = dot_nt(left, one_hot_rows(got[7:8], nz))
        n = len(values) * 16
        return sums[0:n] + sums[n : 2 * n]

    def receive(b):
        got = in_bucket[b]
        sums = sums_of(got, b, True)
        for v in range(5):
            part = sums[v * 16 : (v + 1) * 16]
            if b < 2:
                at = v * cells + (0 if b == 0 else (cx - 1) * cy)
                acc_ref[at : at + cy, :] += part
            else:
                edge = 0 if b == 2 else cy - 1
                for x in range(cx):
                    at = v * cells + x * cy + edge
                    acc_ref[at : at + 1, :] += part[x : x + 1]

    def deposit(v):
        at = slice(v * cells, (v + 1) * cells)
        return (acc_ref[at, :] + low_ref[at, :] * (1.0 / LIFT)).reshape(cx, cy, nz)

    def receive_x():
        wait_received(moves, (0, 1))
        receive(0)
        receive(1)
        for load in loads[5:]:
            load.wait()
        energy = energy_ref[...] + deposit(4)
        for x in range(cx):
            out_face[2, x : x + 1, :] = (ADIABATIC_INDEX - 1.0) * energy[x, 0:1, :]
            out_face[3, x : x + 1, :] = (ADIABATIC_INDEX - 1.0) * energy[x, cy - 1 : cy, :]
        send(faces, (2, 3))

    def receive_y():
        wait_received(moves, (2, 3))
        receive(2)
        receive(3)
        for h in (2, 3):
            own_ref[h - 2] = (ADIABATIC_INDEX - 1.0) * sums_of(out_bucket[h], h, False)
        energy = energy_ref[...] + deposit(4)
        en_ref[...] = energy
        out_face[0] = (ADIABATIC_INDEX - 1.0) * energy[0]
        out_face[1] = (ADIABATIC_INDEX - 1.0) * energy[cx - 1]
        send(faces, (0, 1))

    far = (gy == half - 1) | (gy == half)
    others = slice(0, 4 * cells)
    spread(chunk_of(0), (0, 1, 2, 3), a0_ref, c0_ref)

    def two_others(i, carry):
        pl.when(i == 1)(receive_x)
        pl.when(((i == 2) & jnp.logical_not(far)) | ((i == 3) & far))(receive_y)
        place = chunk_of(i)
        acc_ref[others, :] += dot_nt(a0_ref[...], b0_ref[:, place])
        low_ref[others, :] += dot_nt(c0_ref[...], d0_ref[:, place])
        spread(chunk_of(2 * i + 1), (0, 1, 2, 3), a1_ref, c1_ref)
        acc_ref[others, :] += dot_nt(a1_ref[...], b1_ref[:, place])
        low_ref[others, :] += dot_nt(c1_ref[...], d1_ref[:, place])
        spread(chunk_of(jnp.minimum(2 * i + 2, chunks - 1)), (0, 1, 2, 3), a0_ref, c0_ref)
        return carry

    lax.fori_loop(0, chunks // 2, two_others, 0)

    pressure = (ADIABATIC_INDEX - 1.0) * en_ref[...]
    density = density_ref[...] + deposit(0)
    rho_ref[...] = density
    lane = lax.broadcasted_iota(jnp.int32, (cx, cy, nz), 2)
    after = jnp.where(lane == nz - 1, 0.0, pltpu.roll(pressure, nz - 1, 2))
    before = jnp.where(lane == 0, 0.0, pltpu.roll(pressure, 1, 2))
    impulse_z = momentum_ref[2] + deposit(3) - KICK * (0.5 * (after - before))
    imp_ref[2] = impulse_z
    sound = jnp.sqrt(ADIABATIC_INDEX * pressure / density)
    wait_received(faces, range(4))
    low_x = jnp.where(gx > 0, in_face[0], 0.0)
    high_x = jnp.where(gx < n_gx - 1, in_face[1], 0.0)
    low_y = jnp.where(gy > 0, in_face[2] + own_ref[0], 0.0)
    high_y = jnp.where(gy < n_gy - 1, in_face[3] + own_ref[1], 0.0)
    after = jnp.concatenate([pressure[1:], high_x[None]], axis=0)
    before = jnp.concatenate([low_x[None], pressure[:-1]], axis=0)
    impulse_x = momentum_ref[0] + deposit(1) - KICK * (0.5 * (after - before))
    imp_ref[0] = impulse_x
    line = lax.broadcasted_iota(jnp.int32, (cx, cy, nz), 1)
    after = jnp.where(line == cy - 1, high_y[:, None, :], pltpu.roll(pressure, cy - 1, 1))
    before = jnp.where(line == 0, low_y[:, None, :], pltpu.roll(pressure, 1, 1))
    impulse_y = momentum_ref[1] + deposit(2) - KICK * (0.5 * (after - before))
    imp_ref[1] = impulse_y
    fastest = jnp.maximum(jnp.maximum(jnp.abs(impulse_x), jnp.abs(impulse_y)), jnp.abs(impulse_z))
    wave = fastest / density + sound

    def share_max(me, n, peer, slots, send, recv):
        copies = []
        for k in range(1, n):
            copies.append(pltpu.make_async_remote_copy(
                src_ref=slots.at[me], dst_ref=slots.at[me], send_sem=send.at[k],
                recv_sem=recv.at[k], device_id=peer(k), device_id_type=MESH,
            ))
        return copies

    top = jnp.max(jnp.max(wave, axis=0), axis=0, keepdims=True)
    max_p[plane] = jnp.maximum(top[:, 0:128], top[:, 128:256])
    to_hubs = []
    for n, spot in enumerate(HUBS):
        hub = spot[1] * n_gx + spot[0]
        to_hubs.append((jnp.logical_not(is_at((gx, gy), (spot,))), pltpu.make_async_remote_copy(
            src_ref=max_p.at[plane], dst_ref=max_h.at[lax.rem(me + devices - hub - 1, devices)], send_sem=mh_send.at[n],
            recv_sem=mh_recv.at[0], device_id={"gx": spot[0], "gy": spot[1]}, device_id_type=MESH,
        )))
    for other, copy in to_hubs:
        pl.when(other)(copy.start)
    sent_p = share_max(plane, half, plane_peer, max_p, mp_send, mp_recv)
    for copy in sent_p:
        copy.start()
    stays = col_ref[...] >= 0.0
    state_ref[:, :rows] = jnp.where(stays, pay_ref[0:5, :], 0.0)
    moved_ref[:, :rows] = jnp.where(stays, cell_ref[...], 0)
    for b in range(4):
        state_ref[:, rows + b * cap : rows + (b + 1) * cap] = in_bucket[b, 0:5]
        moved_ref[:, rows + b * cap : rows + (b + 1) * cap] = in_bucket[b, 5:8].astype(jnp.int32)
    for copy in sent_p:
        copy.wait_recv()
    max_z[in_column] = jnp.max(max_p[...], axis=0)
    sent_z = share_max(in_column, n_column, column_peer, max_z, mz_send, mz_recv)
    for k in range(1, n_column):
        peer = column_peer(k)
        to_other = jnp.logical_not(is_at((peer["gx"], peer["gy"]), HUBS))
        pl.when(to_other)(sent_z[k - 1].start)

    @pl.when(not_hub)
    def _():
        for copy in sent_z:
            copy.wait_recv()
        step_ref[...] = COURANT / jnp.broadcast_to(jnp.max(max_z[...]), (1, 128))

    @pl.when(is_hub)
    def _():
        arrived = max_h.at[pl.ds(0, devices - 1)]
        pltpu.make_async_remote_copy(
            src_ref=arrived, dst_ref=arrived, send_sem=mh_send.at[0], recv_sem=mh_recv.at[0],
            device_id={"gx": HUBS[0][0], "gy": HUBS[0][1]}, device_id_type=MESH,
        ).wait_recv()
        best = jnp.maximum(jnp.max(arrived[...], axis=0), max_p[plane])
        step_ref[...] = COURANT / jnp.broadcast_to(jnp.max(best), (1, 128))

    for other, copy in to_hubs:
        pl.when(other)(copy.wait_send)
    for k in range(1, n_column):
        peer = column_peer(k)
        to_other = jnp.logical_not(is_at((peer["gx"], peer["gy"]), HUBS))
        pl.when(to_other)(sent_z[k - 1].wait_send)
    for copies in (moves, faces):
        for h in range(4):
            pl.when(inside[h])(copies[h].wait_send)
    for copy in sent_p:
        copy.wait_send()


def put_out(*refs):
    count = (len(refs) - 2) // 2
    step_ref, sem = refs[-2:]
    step_ref[0] = refs[count - 1][0, 0]
    copies = []
    for k in range(count):
        source = refs[k] if k < count - 1 else step_ref
        copy = pltpu.make_async_copy(source, refs[count + k], sem.at[k])
        copy.start()
        copies.append(copy)
    for copy in copies:
        copy.wait()


def on_device(n_gx, n_gy, density, momentum, energy, mass, velocity, temp, cell, count):
    rows = mass.shape[0]
    cap = rows // 16
    slots = rows + 4 * cap
    cx, cy, nz = density.shape
    vmem = pl.BlockSpec(memory_space=pltpu.VMEM)
    hbm = pl.BlockSpec(memory_space=pltpu.HBM)
    cells = cx * cy
    half = n_gy // 2
    dma = pltpu.SemaphoreType.DMA
    outs = pl.pallas_call(
        functools.partial(kernel, n_gx, n_gy),
        out_shape=(
            pltpu.VMEM(density.shape, F32),
            pltpu.VMEM(momentum.shape, F32),
            pltpu.VMEM(energy.shape, F32),
            pltpu.VMEM((5, slots), F32),
            pltpu.VMEM((3, slots), jnp.int32),
            pltpu.VMEM((1, 128), F32),
        ),
        in_specs=[hbm] * 8,
        out_specs=(vmem,) * 6,
        scratch_shapes=[
            pltpu.VMEM((8, rows), F32),
            pltpu.VMEM((8, rows), F32),
            pltpu.VMEM((1, rows), F32),
            pltpu.VMEM((1, rows), F32),
            pltpu.VMEM((1, rows), F32),
            pltpu.VMEM((4 * (cap // 128) * 16, CHUNK), BF16),
            pltpu.VMEM((4 * (cap // 128) * 16, CHUNK), BF16),
            pltpu.VMEM((128, CHUNK), BF16),
            pltpu.VMEM((128, CHUNK), BF16),
            pltpu.VMEM((4 * cells, CHUNK), BF16),
            pltpu.VMEM((4 * cells, CHUNK), BF16),
            pltpu.VMEM((4 * cells, CHUNK), F8),
            pltpu.VMEM((4 * cells, CHUNK), F8),
            pltpu.VMEM((cells, CHUNK), BF16),
            pltpu.VMEM((cells, CHUNK), BF16),
            pltpu.VMEM((cells, CHUNK), F8),
            pltpu.VMEM((cells, CHUNK), F8),
            pltpu.VMEM((nz, rows // 2), BF16),
            pltpu.VMEM((nz, rows // 2), BF16),
            pltpu.VMEM((nz, rows // 2), F8),
            pltpu.VMEM((nz, rows // 2), F8),
            pltpu.VMEM((5 * cells, nz), F32),
            pltpu.VMEM((5 * cells, nz), F32),
            pltpu.VMEM((4 * (cap // 128) * 16, 128), F32),
            pltpu.VMEM((4, 8, cap), F32),
            pltpu.VMEM((4, 8, cap), F32),
            pltpu.VMEM((4, cx, nz), F32),
            pltpu.VMEM((4, cx, nz), F32),
            pltpu.VMEM((2, cx, nz), F32),
            pltpu.VMEM((2 * n_gx, 1, 128), F32),
            pltpu.VMEM((half, 1, 128), F32),
            pltpu.VMEM((n_gx * n_gy, 1, 128), F32),
            dma((4,)),
            dma((4,)),
            dma((4,)),
            dma((4,)),
            dma((2 * n_gx,)),
            dma((2 * n_gx,)),
            dma((half,)),
            dma((half,)),
            dma((len(HUBS),)),
            dma((1,)),
            pltpu.VMEM((1, 1), jnp.int32),
            pltpu.VMEM(density.shape, F32),
            pltpu.VMEM(momentum.shape, F32),
            pltpu.VMEM(energy.shape, F32),
            pltpu.VMEM((1, rows), F32),
            pltpu.VMEM(velocity.shape, F32),
            pltpu.VMEM((1, rows), F32),
            pltpu.VMEM(cell.shape, jnp.int32),
            dma((8,)),
        ],
        compiler_params=pltpu.CompilerParams(
            collective_id=0, has_side_effects=True, vmem_limit_bytes=64200000
        ),
        name="spray",
    )(count.reshape(1, 1), density, momentum, energy, mass.reshape(1, rows), velocity, temp.reshape(1, rows), cell)
    final = pl.pallas_call(
        put_out,
        out_shape=tuple(pltpu.HBM(o.shape, o.dtype) for o in outs[:5]) + (pltpu.HBM((1,), F32),),
        in_specs=[vmem] * 6,
        out_specs=(hbm,) * 6,
        scratch_shapes=[pltpu.SMEM((1,), F32), dma((6,))],
        compiler_params=pltpu.CompilerParams(vmem_limit_bytes=8 * 1024 * 1024),
        name="put_out",
    )(*outs)
    return tuple(final[:5]) + (final[5].reshape(()),)


def solution(mesh):
    in_specs = (
        P("gx", "gy", None),
        P(None, "gx", "gy", None),
        P("gx", "gy", None),
        P(("gx", "gy")),
        P(None, ("gx", "gy")),
        P(("gx", "gy")),
        P(None, ("gx", "gy")),
        P(("gx", "gy")),
    )
    out_specs = (
        P("gx", "gy", None),
        P(None, "gx", "gy", None),
        P("gx", "gy", None),
        P(None, ("gx", "gy")),
        P(None, ("gx", "gy")),
        P(),
    )
    return jax.shard_map(
        functools.partial(on_device, mesh.shape["gx"], mesh.shape["gy"]),
        mesh=mesh, in_specs=in_specs, out_specs=out_specs, check_vma=False,
    )
```
